32 devices in a mesh: gx: 8 (over y, x, core), gz: 4 (over z).
Axes of the slice: x: 2, y: 2, z: 4, core: 2. Of those that a mesh axis runs over, the one named last changes fastest.
Arguments:
- velocity: float32 [3, 64, 64, 512], P(None, 'gx', None, 'gz'), may hold values from -40 to 40
Outputs:
- coefficient: float32 [64], replicated
- eddy_viscosity: float32 [64, 64, 512], P('gx', None, 'gz')
The draws below stay inside these ranges and needn't reach their ends.
All inputs are finite; a program needn't handle non-finite values.
Results may differ from the reference program's by a relative error of at most 0.0001.
Values sent between devices are 32-bit elements; how exact they have to be, the bound alone decides.
No kernel may reach another device: no remote copies, remote signals or barrier semaphores. Data moves between devices by JAX's collectives and lax.ppermute only.
A program may use at most 64 MiB of HBM per device.

```python
import jax
import jax.numpy as jnp
from jax import lax

NY = 64
NX = 64
NZ = 512


def draw_velocity(key, part):
    key_list = jax.random.split(key, 1)
    x_frac = jnp.arange(NX, dtype=jnp.float32) / NX
    z_frac = jnp.arange(NZ, dtype=jnp.float32) / NZ
    rising = jnp.exp(jnp.log(1.5) * (x_frac[:, None, None] + z_frac[None, None, :]))
    field = jax.random.truncated_normal(key_list[0], -6.0, 6.0, (3, NX, NY, NZ), jnp.float32) * rising
    return field.astype(jnp.float32)


def setup_inputs(seed: int = 0) -> dict:
    keys = jax.random.split(jax.random.key(seed), 2)
    velocity = draw_velocity(jax.random.fold_in(keys[1], 71), 0)
    return dict(velocity=velocity)


index_pairs = ((0, 0), (1, 1), (2, 2), (0, 1), (0, 2), (1, 2))
pair_weights = (1.0, 1.0, 1.0, 2.0, 2.0, 2.0)

def trim_edges(field):
    return field[..., 1:-1, :, 1:-1]

def along_x(field):
    return 0.5 * (field[..., 2:, :, 1:-1] - field[..., :-2, :, 1:-1])

def along_z(field):
    return 0.5 * (field[..., 1:-1, :, 2:] - field[..., 1:-1, :, :-2])

def along_y(field):
    inside = trim_edges(field)
    middle = 0.5 * (inside[..., 2:, :] - inside[..., :-2, :])
    bottom = inside[..., 1:2, :] - inside[..., 0:1, :]
    upper_end = inside[..., -1:, :] - inside[..., -2:-1, :]
    return jnp.concatenate([bottom, middle, upper_end], axis=-2)

def strain(velocity):
    gradients = [along_x(velocity), along_y(velocity), along_z(velocity)]
    strain_rate = jnp.stack([0.5 * (gradients[col_idx][row_idx] + gradients[row_idx][col_idx]) for row_idx, col_idx in index_pairs])
    weights = jnp.array(pair_weights, dtype=jnp.float32)[:, None, None, None]
    magnitude = jnp.sqrt(2.0 * lax.optimization_barrier(jnp.sum(weights * strain_rate * strain_rate, axis=0)))
    return (strain_rate, magnitude)

def box_filter(field):
    streamwise = 0.25 * (field[..., :-2, :, :] + 2.0 * field[..., 1:-1, :, :] + field[..., 2:, :, :])
    return 0.25 * (streamwise[..., :-2] + 2.0 * streamwise[..., 1:-1] + streamwise[..., 2:])

def wrap_pad(field):
    return jnp.pad(field, ((0, 0), (1, 1), (0, 0), (1, 1)), mode='wrap')

def reference(velocity):
    strain_rate, magnitude = strain(wrap_pad(velocity))
    filt_vel = box_filter(wrap_pad(velocity))
    test_rate, test_mag = strain(wrap_pad(filt_vel))
    numer = jnp.zeros((NY,), jnp.float32)
    denom = jnp.zeros((NY,), jnp.float32)
    for slot, (row_idx, col_idx) in enumerate(index_pairs):
        product = (velocity[row_idx] * velocity[col_idx])[None]
        filt_prod = box_filter(wrap_pad(product))[0]
        stress = (magnitude * strain_rate[slot])[None]
        filt_stress = box_filter(wrap_pad(stress))[0]
        leonard = filt_prod - filt_vel[row_idx] * filt_vel[col_idx]
        model_term = 2.0 * (filt_stress - 4.0 * test_mag * test_rate[slot])
        numer = numer + pair_weights[slot] * lax.optimization_barrier(jnp.sum(leonard * model_term, axis=(0, 2)))
        denom = denom + pair_weights[slot] * lax.optimization_barrier(jnp.sum(model_term * model_term, axis=(0, 2)))
    cells = NX * NZ
    coefficient = numer / cells / (denom / cells + 1e-06)
    eddy_viscosity = coefficient[None, :, None] * magnitude
    return (coefficient, eddy_viscosity)
```

```python
import jax
import jax.numpy as jnp
from jax import lax
from jax.sharding import PartitionSpec as P

index_pairs = ((0, 0), (1, 1), (2, 2), (0, 1), (0, 2), (1, 2))
pair_weights = (1.0, 1.0, 1.0, 2.0, 2.0, 2.0)


def swap_edges(low_edge, high_edge, axis):
    count = lax.axis_size(axis)
    if count % 2:
        forward = [(i, (i + 1) % count) for i in range(count)]
        backward = [(target, source) for source, target in forward]
        return (
            lax.ppermute(high_edge, axis, forward),
            lax.ppermute(low_edge, axis, backward),
        )
    odd = lax.axis_index(axis) % 2 == 1
    far_pairs = [(i, (i + 1 if i % 2 else i - 1) % count) for i in range(count)]
    near_pairs = [(i, i ^ 1) for i in range(count)]
    far = lax.ppermute(jnp.where(odd, high_edge, low_edge), axis, far_pairs)
    near = lax.ppermute(jnp.where(odd, low_edge, high_edge), axis, near_pairs)
    return (jnp.where(odd, near, far), jnp.where(odd, far, near))


def extended(block, sides, width):
    for axis, dim in sides:
        low, high = swap_edges(
            lax.slice_in_dim(block, 0, width, axis=dim),
            lax.slice_in_dim(block, block.shape[dim] - width, None, axis=dim),
            axis,
        )
        block = jnp.concatenate([low, block, high], axis=dim)
    return block


def sum_over_devices(partial):
    axes = ("gx", "gz")
    count = lax.axis_size("gx") * lax.axis_size("gz")
    sent = jnp.broadcast_to(partial[None], (count, *partial.shape))
    return jnp.sum(lax.all_to_all(sent, axes, 0, 0, tiled=True), axis=0)


def trim_edges(field):
    return field[..., 1:-1, :, 1:-1]


def along_x(field):
    return 0.5 * (field[..., 2:, :, 1:-1] - field[..., :-2, :, 1:-1])


def along_z(field):
    return 0.5 * (field[..., 1:-1, :, 2:] - field[..., 1:-1, :, :-2])


def along_y(field):
    inside = trim_edges(field)
    middle = 0.5 * (inside[..., 2:, :] - inside[..., :-2, :])
    bottom = inside[..., 1:2, :] - inside[..., 0:1, :]
    upper_end = inside[..., -1:, :] - inside[..., -2:-1, :]
    return jnp.concatenate([bottom, middle, upper_end], axis=-2)


def strain(velocity):
    gradients = [along_x(velocity), along_y(velocity), along_z(velocity)]
    strain_rate = jnp.stack(
        [
            0.5 * (gradients[col_idx][row_idx] + gradients[row_idx][col_idx])
            for row_idx, col_idx in index_pairs
        ]
    )
    weights = jnp.array(pair_weights, dtype=jnp.float32)[:, None, None, None]
    magnitude = jnp.sqrt(2.0 * jnp.sum(weights * strain_rate * strain_rate, axis=0))
    return (strain_rate, magnitude)


def box_filter(field):
    streamwise = 0.25 * (
        field[..., :-2, :, :] + 2.0 * field[..., 1:-1, :, :] + field[..., 2:, :, :]
    )
    return 0.25 * (streamwise[..., :-2] + 2.0 * streamwise[..., 1:-1] + streamwise[..., 2:])


def pair_products(velocity):
    return jnp.stack([velocity[row_idx] * velocity[col_idx] for row_idx, col_idx in index_pairs])


def on_device(velocity):
    wide = extended(velocity, (("gx", 1), ("gz", 3)), 2)
    strain_ext, magnitude_ext = strain(wide)
    filt_prod = box_filter(pair_products(trim_edges(wide)))
    filt_stress = box_filter(magnitude_ext[None] * strain_ext)
    filt_ext = box_filter(wide)
    test_rate, test_mag = strain(filt_ext)
    filt_vel = trim_edges(filt_ext)
    grid_mag = trim_edges(magnitude_ext)
    numer = jnp.zeros((velocity.shape[2],), jnp.float32)
    denom = jnp.zeros((velocity.shape[2],), jnp.float32)
    for slot, (row_idx, col_idx) in enumerate(index_pairs):
        leonard = filt_prod[slot] - filt_vel[row_idx] * filt_vel[col_idx]
        model_term = 2.0 * (filt_stress[slot] - 4.0 * test_mag * test_rate[slot])
        numer = numer + pair_weights[slot] * jnp.sum(leonard * model_term, axis=(0, 2))
        denom = denom + pair_weights[slot] * jnp.sum(model_term * model_term, axis=(0, 2))
    sums = sum_over_devices(jnp.concatenate([numer, denom]))
    numer, denom = jnp.split(sums, 2)
    cells = velocity.shape[1] * lax.axis_size("gx") * velocity.shape[3] * lax.axis_size("gz")
    coefficient = numer / cells / (denom / cells + 1e-06)
    eddy_viscosity = coefficient[None, :, None] * grid_mag
    return (coefficient, eddy_viscosity)


def solution(mesh):
    in_specs = (P(None, "gx", None, "gz"),)
    out_specs = (P(), P("gx", None, "gz"))
    return jax.shard_map(
        on_device, mesh=mesh, in_specs=in_specs, out_specs=out_specs, check_vma=False
    )
```

```python
import functools

import jax
import jax.numpy as jnp
from jax import lax
from jax.experimental import pallas as pl
from jax.experimental.pallas import tpu as pltpu
from jax.sharding import PartitionSpec as P

WIDTH = 2
ROWS = 8
index_pairs = ((0, 0), (1, 1), (2, 2), (0, 1), (0, 2), (1, 2))
TOP = 9

VMEM = pl.BlockSpec(memory_space=pltpu.VMEM)


def swap_pairs(count):
    far = [(i, (i + 1 if i % 2 else i - 1) % count) for i in range(count)]
    near = [(i, i ^ 1) for i in range(count)]
    return far, near


def swap_edges(for_below, for_above, axis):
    count = lax.axis_size(axis)
    if count % 2:
        forward = [(i, (i + 1) % count) for i in range(count)]
        backward = [(target, source) for source, target in forward]
        return (
            lax.ppermute(for_above, axis, forward),
            lax.ppermute(for_below, axis, backward),
        )
    odd = lax.axis_index(axis) % 2 == 1
    far_pairs, near_pairs = swap_pairs(count)
    far = lax.ppermute(jnp.where(odd, for_above, for_below), axis, far_pairs)
    near = lax.ppermute(jnp.where(odd, for_below, for_above), axis, near_pairs)
    return (jnp.where(odd, near, far), jnp.where(odd, far, near))


def to_folded(plane):
    half = plane.shape[1] // 2
    return jnp.concatenate([plane[:, :half], plane[:, half:]], axis=0).T


def from_folded(folded):
    ny = folded.shape[1] // 2
    turned = folded.T
    return jnp.concatenate([turned[:ny], turned[ny:]], axis=1)


def fold_kernel(vel_ref, below_ref, above_ref, u_ref, edge_ref):
    nx, ny, nz = vel_ref.shape[1:]
    half = nz // 2
    lower = lax.broadcasted_iota(jnp.int32, (WIDTH, 2 * ny), 1) < ny

    def put(comp, slot, plane):
        folded = to_folded(plane)
        u_ref[comp, slot] = folded
        edge_ref[comp, slot] = jnp.where(lower, folded[:WIDTH], folded[half - WIDTH :])

    for comp in range(3):
        for layer in range(WIDTH):
            put(comp, layer, below_ref[comp, layer])
            put(comp, WIDTH + nx + layer, above_ref[comp, layer])

        def step(x, carry):
            put(comp, WIDTH + x, vel_ref[comp, x])
            return carry

        lax.fori_loop(0, nx, step, 0)


def slope_along_lanes(field, first, last, scale):
    lanes = field.shape[1]
    up = jnp.where(last, field, pltpu.roll(field, lanes - 1, 1))
    down = jnp.where(first, field, pltpu.roll(field, 1, 1))
    return (up - down) * scale


def rates(slopes):
    rate = [
        slopes[i][i] if i == j else slopes[i][j] + slopes[j][i] for i, j in index_pairs
    ]
    squares = [r * r for r in rate]
    straight = squares[0] + squares[1] + squares[2]
    crossed = squares[3] + squares[4] + squares[5]
    return rate, 0.5 * jnp.sqrt((straight + straight) + crossed)


def weighted(low, mid, high):
    return (low + high) + (mid + mid)


def main_kernel(
    u_ref, low_ref, high_ref, mag_ref, sums_ref, ue, tmp, fz, hz, hu, mag
):
    planes, half, lanes = u_ref.shape[1:]
    nx = planes - 2 * WIDTH
    ny = lanes // 2
    zero = jnp.minimum(lax.axis_index("gx"), 0)
    lane = lax.broadcasted_iota(jnp.int32, (ROWS, lanes), 1)
    row_y = lax.rem(lane, ny)
    first, last = row_y == 0, row_y == ny - 1
    scale = jnp.where(first | last, 2.0, 1.0).astype(jnp.float32)
    upper = lax.broadcasted_iota(jnp.int32, (WIDTH, lanes), 1) >= ny

    def rows(start, count=ROWS):
        return pl.ds(zero + start, count)

    def fill(x, carry):
        for comp in range(3):
            for k in range(half // ROWS):
                ue[comp, x, rows(TOP + ROWS * k)] = u_ref[comp, x, ROWS * k : ROWS * (k + 1)]
            below = jnp.where(upper, low_ref[comp, x], u_ref[comp, x, half - WIDTH :])
            above = jnp.where(upper, u_ref[comp, x, :WIDTH], high_ref[comp, x])
            ue[comp, x, rows(TOP - WIDTH, WIDTH)] = pltpu.roll(below, ny, 1)
            ue[comp, x, rows(TOP + half, WIDTH)] = pltpu.roll(above, ny, 1)
        return carry

    lax.fori_loop(0, planes, fill, 0)
    windows = half // ROWS + 1

    def filter_z(x, k, comp):
        at = TOP - 1 + ROWS * k
        return weighted(
            ue[comp, x, rows(at - 1)], ue[comp, x, rows(at)], ue[comp, x, rows(at + 1)]
        )

    for x in (0, planes - 1):
        for k in range(windows):
            for comp in range(3):
                hz[comp, x, ROWS * k : ROWS * (k + 1)] = filter_z(x, k, comp)

    def strain_plane(i, carry):
        for k in range(windows):
            at = TOP - 1 + ROWS * k
            here = pl.ds(ROWS * k, ROWS)
            mid = [ue[comp, i + 1, rows(at)] for comp in range(3)]
            after = [ue[comp, i + 1, rows(at + 1)] for comp in range(3)]
            before = [ue[comp, i + 1, rows(at - 1)] for comp in range(3)]
            slopes = [
                (
                    ue[comp, i + 2, rows(at)] - ue[comp, i, rows(at)],
                    slope_along_lanes(mid[comp], first, last, scale),
                    after[comp] - before[comp],
                )
                for comp in range(3)
            ]
            rate, size = rates(slopes)
            mag[i, here] = size
            scaled = size * 0.0625
            quarter = [0.25 * m for m in mid]
            for n, (a, b) in enumerate(index_pairs):
                tmp[n, here] = scaled * rate[n]
                tmp[6 + n, here] = quarter[a] * quarter[b]
            for comp in range(3):
                hz[comp, i + 1, here] = weighted(before[comp], mid[comp], after[comp])
        for n in range(12):
            for k in range(half // ROWS):
                fz[n, i, ROWS * k : ROWS * (k + 1)] = weighted(
                    tmp[n, rows(ROWS * k)], tmp[n, rows(ROWS * k + 1)], tmp[n, rows(ROWS * k + 2)]
                )
        return carry

    lax.fori_loop(0, nx + 2, strain_plane, 0)

    def hat_plane(i, carry):
        for comp in range(3):
            for k in range(windows):
                here = pl.ds(ROWS * k, ROWS)
                hu[comp, i, here] = 0.0625 * weighted(
                    hz[comp, i, here], hz[comp, i + 1, here], hz[comp, i + 2, here]
                )
        return carry

    lax.fori_loop(0, nx + 2, hat_plane, 0)

    def sum_plane(x, carry):
        numer, denom = carry
        for k in range(half // ROWS):
            at = 1 + ROWS * k
            here = pl.ds(ROWS * k, ROWS)
            mid = [hu[comp, x + 1, rows(at)] for comp in range(3)]
            slopes = [
                (
                    hu[comp, x + 2, rows(at)] - hu[comp, x, rows(at)],
                    slope_along_lanes(mid[comp], first, last, scale),
                    hu[comp, x + 1, rows(at + 1)] - hu[comp, x + 1, rows(at - 1)],
                )
                for comp in range(3)
            ]
            rate, size = rates(slopes)
            size = 4.0 * size
            top, straight, crossed = [], [], []
            for n, (a, b) in enumerate(index_pairs):
                stress = weighted(fz[n, x, here], fz[n, x + 1, here], fz[n, x + 2, here])
                product = weighted(
                    fz[6 + n, x, here], fz[6 + n, x + 1, here], fz[6 + n, x + 2, here]
                )
                model = stress - size * rate[n]
                leonard = product - mid[a] * mid[b]
                top.append(leonard * model)
                (straight if a == b else crossed).append(model * model)
            numer = numer + ((top[0] + top[1]) + (top[2] + top[3]) + (top[4] + top[5]))
            denom = denom + (
                (straight[0] + straight[1] + straight[2])
                + 0.5 * (crossed[0] + crossed[1] + crossed[2])
            )
        mag_ref[x] = from_folded(mag[x + 1, rows(1, half)])
        return numer, denom

    start = jnp.zeros((ROWS, lanes), jnp.float32)
    numer, denom = lax.fori_loop(0, nx, sum_plane, (start, start))
    numer = jnp.sum(numer, axis=0, keepdims=True)
    denom = jnp.sum(denom, axis=0, keepdims=True)
    numer = numer + pltpu.roll(numer, ny, 1)
    denom = denom + pltpu.roll(denom, ny, 1)
    both = jnp.where(lax.broadcasted_iota(jnp.int32, (1, lanes), 1) < ny, numer, denom)
    sums_ref[...] = jnp.broadcast_to(both, sums_ref.shape)


def finish_kernel(cells, parts_ref, mag_ref, coefficient_ref, eddy_ref):
    lanes = parts_ref.shape[1]
    ny = lanes // 2
    sums = jnp.sum(parts_ref[...], axis=0, keepdims=True)
    numer = sums[:, :ny]
    denom = pltpu.roll(sums, ny, 1)[:, :ny]
    coefficient = numer / cells / (denom / cells + 1e-06)
    coefficient_ref[...] = coefficient
    column = jnp.broadcast_to(coefficient, (mag_ref.shape[2], ny)).T
    for x in range(mag_ref.shape[0]):
        eddy_ref[x] = column * mag_ref[x]


def on_device(velocity):
    nx, ny, nz = velocity.shape[1:]
    half, lanes = nz // 2, 2 * ny
    planes = nx + 2 * WIDTH
    f32 = jnp.float32
    params = pltpu.CompilerParams(vmem_limit_bytes=24 * 1024 * 1024)

    below, above = swap_edges(velocity[:, :WIDTH], velocity[:, nx - WIDTH :], "gx")
    folded, edges = pl.pallas_call(
        fold_kernel,
        out_shape=(
            jax.ShapeDtypeStruct((3, planes, half, lanes), f32),
            jax.ShapeDtypeStruct((3, planes, WIDTH, lanes), f32),
        ),
        in_specs=[VMEM] * 3,
        out_specs=(VMEM, VMEM),
        compiler_params=params,
        name="fold",
    )(velocity, below, above)
    low, high = swap_edges(edges, edges, "gz")
    count = lax.axis_size("gx") * lax.axis_size("gz")
    tall = half + 3 * ROWS
    windowed = half + ROWS
    magnitude, sums = pl.pallas_call(
        main_kernel,
        out_shape=(
            jax.ShapeDtypeStruct((nx, ny, nz), f32),
            jax.ShapeDtypeStruct((count, lanes), f32),
        ),
        in_specs=[VMEM] * 3,
        out_specs=(VMEM, VMEM),
        scratch_shapes=[
            pltpu.VMEM((3, planes, tall, lanes), f32),
            pltpu.VMEM((12, windowed + ROWS, lanes), f32),
            pltpu.VMEM((12, nx + 2, half, lanes), f32),
            pltpu.VMEM((3, planes, windowed, lanes), f32),
            pltpu.VMEM((3, nx + 2, windowed, lanes), f32),
            pltpu.VMEM((nx + 2, windowed, lanes), f32),
        ],
        compiler_params=params,
        name="model",
    )(folded, low, high)
    parts = lax.all_to_all(sums, ("gx", "gz"), 0, 0, tiled=True)
    cells = nx * lax.axis_size("gx") * nz * lax.axis_size("gz")
    coefficient, eddy_viscosity = pl.pallas_call(
        functools.partial(finish_kernel, cells),
        out_shape=(
            jax.ShapeDtypeStruct((1, ny), f32),
            jax.ShapeDtypeStruct((nx, ny, nz), f32),
        ),
        in_specs=[VMEM] * 2,
        out_specs=(VMEM, VMEM),
        compiler_params=params,
        name="finish",
    )(parts, magnitude)
    return (coefficient[0], eddy_viscosity)


def solution(mesh):
    in_specs = (P(None, "gx", None, "gz"),)
    out_specs = (P(), P("gx", None, "gz"))
    return jax.shard_map(
        on_device, mesh=mesh, in_specs=in_specs, out_specs=out_specs, check_vma=False
    )
```

```python
import functools

import jax
import jax.numpy as jnp
from jax import lax
from jax.experimental import pallas as pl
from jax.experimental.pallas import tpu as pltpu
from jax.sharding import PartitionSpec as P

WIDTH = 2
ROWS = 8
index_pairs = ((0, 0), (1, 1), (2, 2), (0, 1), (0, 2), (1, 2))
TOP = 9
SHARED = pltpu.CompilerParams(vmem_limit_bytes=8 * 1024 * 1024)

VMEM = pl.BlockSpec(memory_space=pltpu.VMEM)


def swap_pairs(count):
    far = [(i, (i + 1 if i % 2 else i - 1) % count) for i in range(count)]
    near = [(i, i ^ 1) for i in range(count)]
    return far, near


def swap_edges(for_below, for_above, axis):
    count = lax.axis_size(axis)
    if count % 2:
        forward = [(i, (i + 1) % count) for i in range(count)]
        backward = [(target, source) for source, target in forward]
        return (
            lax.ppermute(for_above, axis, forward),
            lax.ppermute(for_below, axis, backward),
        )
    far_pairs, near_pairs = swap_pairs(count)
    if for_below is for_above:
        near_send = far_send = for_below
    else:
        odd = lax.axis_index(axis) % 2 == 1
        far_send = jnp.where(odd, for_above, for_below)
        near_send = jnp.where(odd, for_below, for_above)
    far = lax.ppermute(far_send, axis, far_pairs)
    near = lax.ppermute(near_send, axis, near_pairs)
    return near, far


def below_is_first(axis):
    if lax.axis_size(axis) % 2:
        return True
    return lax.rem(lax.axis_index(axis), 2) == 1


def mirrored(plane):
    lanes = plane.shape[1]
    lane = lax.broadcasted_iota(jnp.int32, plane.shape, 1)
    return jnp.take_along_axis(plane, lanes - 1 - lane, axis=1)


def to_folded(plane):
    half = plane.shape[1] // 2
    return jnp.concatenate([plane[:, :half], mirrored(plane)[:, :half]], axis=0).T


def from_folded(folded):
    half, lanes = folded.shape
    ny = lanes // 2
    turned = folded.T
    both = jnp.concatenate([turned[:ny], turned[ny:]], axis=1)
    lane = lax.broadcasted_iota(jnp.int32, both.shape, 1)
    return jnp.take_along_axis(both, jnp.where(lane < half, lane, 3 * half - 1 - lane), axis=1)


class Lanes:
    def __init__(self, lanes):
        self.zero = jnp.minimum(lax.axis_index("gx"), 0)
        lane = lax.broadcasted_iota(jnp.int32, (ROWS, lanes), 1)
        row_y = lax.rem(lane, lanes // 2)
        self.first, self.last = row_y == 0, row_y == lanes // 2 - 1
        self.scale = jnp.where(self.first | self.last, 2.0, 1.0).astype(jnp.float32)
        self.sign = jnp.where(lane < lanes // 2, 1.0, -1.0).astype(jnp.float32)

    def rows(self, start, count=ROWS):
        return pl.ds(self.zero + start, count)

    def slope_y(self, field):
        lanes = field.shape[1]
        up = jnp.where(self.last, field, pltpu.roll(field, lanes - 1, 1))
        down = jnp.where(self.first, field, pltpu.roll(field, 1, 1))
        return (up - down) * self.scale

    def slope_z(self, after, before):
        return (after - before) * self.sign


def window(k):
    return pl.ds(ROWS * k, ROWS)


def store_plane(ln, u_ref, comp, slot, plane):
    folded = to_folded(plane)
    half, lanes = folded.shape
    for k in range(half // ROWS):
        u_ref[comp, slot, ln.rows(TOP + ROWS * k)] = folded[ROWS * k : ROWS * (k + 1)]
    inner = pltpu.roll(folded[half - ROWS :], lanes // 2, 1)
    for layer in range(WIDTH):
        u_ref[comp, slot, ln.rows(TOP + half + layer, 1)] = inner[ROWS - 1 - layer : ROWS - layer]


def rates(slopes):
    rate = [
        slopes[i][i] if i == j else slopes[i][j] + slopes[j][i] for i, j in index_pairs
    ]
    squares = [r * r for r in rate]
    straight = squares[0] + squares[1] + squares[2]
    crossed = squares[3] + squares[4] + squares[5]
    return rate, 0.5 * jnp.sqrt((straight + straight) + crossed)


def weighted(low, mid, high):
    return (low + high) + (mid + mid)


def filter_z(ln, u_ref, hz_ref, slot, k):
    at = ROWS * (k + 1)
    for comp in range(3):
        hz_ref[comp, slot, window(k)] = weighted(
            *[u_ref[comp, slot, ln.rows(at + step)] for step in (-1, 0, 1)]
        )


def strain(ln, u_ref, mag_ref, tmp_ref, keep_ref, slot, i, k):
    at = ROWS * (k + 1)
    mid = [u_ref[comp, i + 1, ln.rows(at)] for comp in range(3)]
    slopes = [
        (
            u_ref[comp, i + 2, ln.rows(at)] - u_ref[comp, i, ln.rows(at)],
            ln.slope_y(mid[comp]),
            ln.slope_z(u_ref[comp, i + 1, ln.rows(at + 1)], u_ref[comp, i + 1, ln.rows(at - 1)]),
        )
        for comp in range(3)
    ]
    rate, size = rates(slopes)
    mag_ref[i, window(k)] = size
    scaled = size * 0.0625
    quarter = [0.25 * m for m in mid]
    for n, (a, b) in enumerate(index_pairs):
        for at, value in ((n, scaled * rate[n]), (6 + n, quarter[a] * quarter[b])):
            tmp_ref[at, slot, window(k)] = value
            if k == 1:
                keep_ref[at, i] = value


def filter_products(ln, tmp_ref, fz_ref, slot, i, k):
    for n in range(12):
        fz_ref[n, i, window(k)] = weighted(
            *[tmp_ref[n, slot, ln.rows(ROWS * k + step)] for step in (0, 1, 2)]
        )


def filter_x(hz_ref, hu_ref, i, k):
    for comp in range(3):
        hu_ref[comp, i, window(k)] = 0.0625 * weighted(
            *[hz_ref[comp, i + step, window(k)] for step in (0, 1, 2)]
        )


def add_sums(ln, hu_ref, fz_ref, x, k, carry):
    numer, denom = carry
    at = 1 + ROWS * k
    mid = [hu_ref[comp, x + 1, ln.rows(at)] for comp in range(3)]
    slopes = [
        (
            hu_ref[comp, x + 2, ln.rows(at)] - hu_ref[comp, x, ln.rows(at)],
            ln.slope_y(mid[comp]),
            ln.slope_z(
                hu_ref[comp, x + 1, ln.rows(at + 1)], hu_ref[comp, x + 1, ln.rows(at - 1)]
            ),
        )
        for comp in range(3)
    ]
    rate, size = rates(slopes)
    size = 4.0 * size
    top, straight, crossed = [], [], []
    for n, (a, b) in enumerate(index_pairs):
        stress = weighted(*[fz_ref[n, x + step, window(k)] for step in (0, 1, 2)])
        product = weighted(*[fz_ref[6 + n, x + step, window(k)] for step in (0, 1, 2)])
        model = stress - size * rate[n]
        leonard = product - mid[a] * mid[b]
        top.append(leonard * model)
        (straight if a == b else crossed).append(model * model)
    numer = numer + ((top[0] + top[1]) + (top[2] + top[3]) + (top[4] + top[5]))
    denom = denom + (
        (straight[0] + straight[1] + straight[2])
        + 0.5 * (crossed[0] + crossed[1] + crossed[2])
    )
    return numer, denom


def strain_planes(ln, u_ref, mag_ref, tmp_ref, keep_ref, fz_ref, start, stop):
    windows = mag_ref.shape[1] // ROWS

    def plane(i):
        for k in range(1, windows):
            strain(ln, u_ref, mag_ref, tmp_ref, keep_ref, lax.rem(i, 2), i, k)

    def products(i):
        for k in range(1, windows - 1):
            filter_products(ln, tmp_ref, fz_ref, lax.rem(i, 2), i, k)

    def step(i, carry):
        products(i - 1)
        plane(i)
        return carry

    plane(start)
    lax.fori_loop(start + 1, stop, step, 0)
    products(stop - 1)


def sum_planes(ln, hu_ref, fz_ref, acc_ref, start, stop):
    def step(x, carry):
        for k in range(1, fz_ref.shape[2] // ROWS):
            carry = add_sums(ln, hu_ref, fz_ref, x, k, carry)
        return carry

    acc_ref[0], acc_ref[1] = lax.fori_loop(start, stop, step, (acc_ref[0], acc_ref[1]))


def interior_kernel(
    vel_ref, u_ref, keep_ref, fz_ref, hz_ref, hu_ref, mag_ref, acc_ref, tmp_ref
):
    nx = vel_ref.shape[1]
    windows = mag_ref.shape[1] // ROWS
    ln = Lanes(u_ref.shape[3])

    def fold(x, carry):
        for comp in range(3):
            store_plane(ln, u_ref, comp, WIDTH + x, vel_ref[comp, x])
        return carry

    lax.fori_loop(0, nx, fold, 0, unroll=2)

    def hat_z(x, carry):
        for k in range(1, windows):
            filter_z(ln, u_ref, hz_ref, WIDTH + x, k)
        return carry

    lax.fori_loop(0, nx, hat_z, 0)

    def hat_x(i, carry):
        for k in range(1, windows):
            filter_x(hz_ref, hu_ref, i, k)
        return carry

    lax.fori_loop(2, nx, hat_x, 0)
    strain_planes(ln, u_ref, mag_ref, tmp_ref, keep_ref, fz_ref, 2, nx)
    acc_ref[...] = jnp.zeros_like(acc_ref)
    sum_planes(ln, hu_ref, fz_ref, acc_ref, 2, nx - 2)


def fold_kernel(first_ref, second_ref, _, u_ref, edge_ref):
    planes = u_ref.shape[1]
    ln = Lanes(u_ref.shape[3])
    ordered = below_is_first("gx")
    for comp in range(3):
        for layer in range(WIDTH):
            first, second = first_ref[comp, layer], second_ref[comp, layer]
            below, above = jnp.where(ordered, first, second), jnp.where(ordered, second, first)
            store_plane(ln, u_ref, comp, layer, below)
            store_plane(ln, u_ref, comp, planes - WIDTH + layer, above)
    for comp in range(3):
        for slot in range(planes):
            for layer in range(WIDTH):
                to = WIDTH * (comp * planes + slot) + WIDTH - 1 - layer
                edge_ref[to : to + 1] = u_ref[comp, slot, ln.rows(TOP + layer, 1)]


def sides_kernel(
    u_ref, _1, _2, _3, _4, _5, _6,
    keep_ref, fz_ref, hz_ref, hu_ref, mag_ref, acc_ref, tmp_ref,
):
    planes = u_ref.shape[1]
    nx = planes - 2 * WIDTH
    windows = mag_ref.shape[1] // ROWS
    ln = Lanes(u_ref.shape[3])
    for start, stop in ((0, WIDTH), (planes - WIDTH, planes)):
        for slot in range(start, stop):
            for k in range(1, windows):
                filter_z(ln, u_ref, hz_ref, slot, k)
    for start, stop in ((0, 2), (nx, nx + 2)):
        for i in range(start, stop):
            for k in range(1, windows):
                filter_x(hz_ref, hu_ref, i, k)
        strain_planes(ln, u_ref, mag_ref, tmp_ref, keep_ref, fz_ref, start, stop)
    sum_planes(ln, hu_ref, fz_ref, acc_ref, 0, 2)
    sum_planes(ln, hu_ref, fz_ref, acc_ref, nx - 2, nx)


def rim_kernel(
    u_ref, first_ref, second_ref, keep_in, hu_in, mag_in, acc_in,
    mag_ref, sums_ref, near, turned, tmp, fz, hz, hu, mag,
):
    planes, _, lanes = u_ref.shape[1:]
    nx = planes - 2 * WIDTH
    ny = lanes // 2
    ln = Lanes(lanes)
    upper = lax.broadcasted_iota(jnp.int32, first_ref.shape, 1) >= ny
    take_first = jnp.logical_not(jnp.logical_xor(upper, below_is_first("gz")))
    turned[...] = pltpu.roll(jnp.where(take_first, first_ref[...], second_ref[...]), ny, 1)
    for comp in range(3):
        for slot in range(planes):
            at = WIDTH * (comp * planes + slot)
            near[comp, slot, ln.rows(TOP - WIDTH, WIDTH)] = turned[at : at + WIDTH]
            near[comp, slot, ln.rows(TOP)] = u_ref[comp, slot, ln.rows(TOP)]
    for slot in range(planes):
        filter_z(ln, near, hz, slot, 0)
    for i in range(nx + 2):
        strain(ln, near, mag, tmp, None, i, i, 0)
        for n in range(12):
            tmp[n, i, window(1)] = keep_in[n, i]
    for i in range(nx + 2):
        filter_x(hz, hu, i, 0)
        for comp in range(3):
            hu[comp, i, window(1)] = hu_in[comp, i, window(1)]
        filter_products(ln, tmp, fz, i, i, 0)
    carry = acc_in[0], acc_in[1]
    for x in range(nx):
        carry = add_sums(ln, hu, fz, x, 0, carry)
    numer, denom = [jnp.sum(part, axis=0, keepdims=True) for part in carry]
    numer = numer + pltpu.roll(numer, ny, 1)
    denom = denom + pltpu.roll(denom, ny, 1)
    both = jnp.where(lax.broadcasted_iota(jnp.int32, (1, lanes), 1) < ny, numer, denom)
    sums_ref[...] = jnp.broadcast_to(both, sums_ref.shape)
    half = mag_ref.shape[2] // 2
    for x in range(nx):
        mag[x + 1, window(1)] = mag_in[x + 1, window(1)]
        folded = jnp.concatenate(
            [mag[x + 1, ln.rows(1)]]
            + [mag_in[x + 1, ln.rows(1 + ROWS * k)] for k in range(1, half // ROWS)],
            axis=0,
        )
        mag_ref[x] = from_folded(folded)


def finish_kernel(cells, parts_ref, mag_ref, coefficient_ref, eddy_ref):
    lanes = parts_ref.shape[1]
    ny = lanes // 2
    sums = jnp.sum(parts_ref[...], axis=0, keepdims=True)
    numer = sums[:, :ny]
    denom = pltpu.roll(sums, ny, 1)[:, :ny]
    coefficient = numer / cells / (denom / cells + 1e-06)
    coefficient_ref[...] = coefficient
    column = jnp.broadcast_to(coefficient, (mag_ref.shape[2], ny)).T
    for x in range(mag_ref.shape[0]):
        eddy_ref[x] = column * mag_ref[x]


def call(kernel, name, shapes, operands, cycles, aliases=None, scratch=()):
    return pl.pallas_call(
        kernel,
        out_shape=tuple(jax.ShapeDtypeStruct(shape, jnp.float32) for shape in shapes),
        in_specs=[VMEM] * len(operands),
        out_specs=tuple(VMEM for _ in shapes),
        scratch_shapes=[pltpu.VMEM(shape, jnp.float32) for shape in scratch],
        input_output_aliases=aliases or {},
        compiler_params=SHARED,
        cost_estimate=pl.CostEstimate(
            flops=cycles * 4096, bytes_accessed=0, transcendentals=0
        ),
        name=name,
    )(*operands)


def on_device(velocity):
    nx, ny, nz = velocity.shape[1:]
    half, lanes = nz // 2, 2 * ny
    planes = nx + 2 * WIDTH
    tall, windowed = half + 3 * ROWS, half + ROWS
    u_shape = (3, planes, tall, lanes)
    work = (
        (12, nx + 2, ROWS, lanes),
        (12, nx + 2, half, lanes),
        (3, planes, windowed, lanes),
        (3, nx + 2, windowed, lanes),
        (nx + 2, windowed, lanes),
        (2, ROWS, lanes),
    )
    window_pair = ((12, 2, windowed, lanes),)
    sent = velocity[:, :WIDTH], velocity[:, nx - WIDTH :]
    first, second = swap_edges(*sent, "gx")
    u, *fields = call(
        interior_kernel, "interior", (u_shape, *work), (velocity,), 6000, scratch=window_pair
    )
    edge_shape = (3 * planes * WIDTH, lanes)
    u, edges = call(
        fold_kernel, "fold", (u_shape, edge_shape), (first, second, u), 800, {2: 0}
    )
    first, second = swap_edges(edges, edges, "gz")
    keep, _, _, hu, mag, acc = call(
        sides_kernel,
        "sides",
        work,
        (u, *fields),
        4000,
        {1 + n: n for n in range(6)},
        window_pair,
    )
    count = lax.axis_size("gx") * lax.axis_size("gz")
    magnitude, sums = call(
        rim_kernel,
        "rim",
        ((nx, ny, nz), (count, lanes)),
        (u, first, second, keep, hu, mag, acc),
        1000,
        scratch=(
            (3, planes, 3 * ROWS, lanes),
            edge_shape,
            (12, nx + 2, 2 * ROWS, lanes),
            (12, nx + 2, ROWS, lanes),
            (3, planes, ROWS, lanes),
            (3, nx + 2, 2 * ROWS, lanes),
            (nx + 2, 2 * ROWS, lanes),
        ),
    )
    parts = lax.all_to_all(sums, ("gx", "gz"), 0, 0, tiled=True)
    cells = nx * lax.axis_size("gx") * nz * lax.axis_size("gz")
    coefficient, eddy_viscosity = call(
        functools.partial(finish_kernel, cells),
        "finish",
        ((1, ny), (nx, ny, nz)),
        (parts, magnitude),
        500,
    )
    return (coefficient[0], eddy_viscosity)


def solution(mesh):
    in_specs = (P(None, "gx", None, "gz"),)
    out_specs = (P(), P("gx", None, "gz"))
    return jax.shard_map(
        on_device, mesh=mesh, in_specs=in_specs, out_specs=out_specs, check_vma=False
    )
```

```python
import functools

import jax
import jax.numpy as jnp
from jax import lax
from jax.experimental import pallas as pl
from jax.experimental.pallas import tpu as pltpu
from jax.sharding import PartitionSpec as P

WIDTH = 2
ROWS = 8
index_pairs = ((0, 0), (1, 1), (2, 2), (0, 1), (0, 2), (1, 2))
TOP = 9

VMEM = pl.BlockSpec(memory_space=pltpu.VMEM)


def swap_pairs(count):
    far = [(i, (i + 1 if i % 2 else i - 1) % count) for i in range(count)]
    near = [(i, i ^ 1) for i in range(count)]
    return far, near


def swap_edges(first, second, axis):
    count = lax.axis_size(axis)
    if count % 2:
        forward = [(i, (i + 1) % count) for i in range(count)]
        backward = [(target, source) for source, target in forward]
        return lax.ppermute(first, axis, forward), lax.ppermute(second, axis, backward)
    far_pairs, near_pairs = swap_pairs(count)
    far = lax.ppermute(second, axis, far_pairs)
    return lax.ppermute(first, axis, near_pairs), far


def below_is_first(axis):
    if lax.axis_size(axis) % 2:
        return True
    return lax.rem(lax.axis_index(axis), 2) == 1


def first_goes_below(axis):
    if lax.axis_size(axis) % 2:
        return False
    return below_is_first(axis)


def mirrored(plane):
    lanes = plane.shape[1]
    lane = lax.broadcasted_iota(jnp.int32, plane.shape, 1)
    return jnp.take_along_axis(plane, lanes - 1 - lane, axis=1)


def to_folded(plane, rows):
    return jnp.concatenate([plane[:, :rows], mirrored(plane)[:, :rows]], axis=0).T


def from_folded(folded):
    half, lanes = folded.shape
    ny = lanes // 2
    turned = folded.T
    both = jnp.concatenate([turned[:ny], turned[ny:]], axis=1)
    lane = lax.broadcasted_iota(jnp.int32, both.shape, 1)
    return jnp.take_along_axis(both, jnp.where(lane < half, lane, 3 * half - 1 - lane), axis=1)


class Lanes:
    def __init__(self, lanes):
        self.zero = jnp.minimum(lax.axis_index("gx"), 0)
        lane = lax.broadcasted_iota(jnp.int32, (ROWS, lanes), 1)
        row_y = lax.rem(lane, lanes // 2)
        self.first, self.last = row_y == 0, row_y == lanes // 2 - 1
        self.scale = jnp.where(self.first | self.last, 2.0, 1.0).astype(jnp.float32)
        self.sign = jnp.where(lane < lanes // 2, 1.0, -1.0).astype(jnp.float32)

    def rows(self, start, count=ROWS):
        return pl.ds(self.zero + start, count)

    def slope_y(self, field):
        lanes = field.shape[1]
        up = jnp.where(self.last, field, pltpu.roll(field, lanes - 1, 1))
        down = jnp.where(self.first, field, pltpu.roll(field, 1, 1))
        return (up - down) * self.scale

    def slope_z(self, after, before):
        return (after - before) * self.sign


def window(k):
    return pl.ds(ROWS * k, ROWS)


def store_plane(ln, u_ref, comp, slot, plane):
    count = plane.shape[1] // 2 + ROWS
    folded = to_folded(plane, count)
    for k in range(count // ROWS):
        u_ref[comp, slot, ln.rows(TOP + ROWS * k)] = folded[ROWS * k : ROWS * (k + 1)]


def rates(slopes):
    rate = [
        slopes[i][i] if i == j else slopes[i][j] + slopes[j][i] for i, j in index_pairs
    ]
    squares = [r * r for r in rate]
    straight = squares[0] + squares[1] + squares[2]
    crossed = squares[3] + squares[4] + squares[5]
    return rate, 0.5 * jnp.sqrt((straight + straight) + crossed)


def weighted(low, mid, high):
    return (low + high) + (mid + mid)


def filter_z(ln, u_ref, hz_ref, slot, k):
    at = ROWS * (k + 1)
    for comp in range(3):
        hz_ref[comp, slot, window(k)] = weighted(
            *[u_ref[comp, slot, ln.rows(at + step)] for step in (-1, 0, 1)]
        )


def strain(ln, u_ref, mag_ref, tmp_ref, keep_ref, slot, i, k):
    at = ROWS * (k + 1)
    mid = [u_ref[comp, i + 1, ln.rows(at)] for comp in range(3)]
    slopes = [
        (
            u_ref[comp, i + 2, ln.rows(at)] - u_ref[comp, i, ln.rows(at)],
            ln.slope_y(mid[comp]),
            ln.slope_z(u_ref[comp, i + 1, ln.rows(at + 1)], u_ref[comp, i + 1, ln.rows(at - 1)]),
        )
        for comp in range(3)
    ]
    rate, size = rates(slopes)
    mag_ref[i, window(k)] = size
    scaled = size * 0.0625
    quarter = [0.25 * m for m in mid]
    for n, (a, b) in enumerate(index_pairs):
        for at, value in ((n, scaled * rate[n]), (6 + n, quarter[a] * quarter[b])):
            tmp_ref[at, slot, window(k)] = value
            if k == 1:
                keep_ref[at, i, window(1)] = value


def filter_products(ln, tmp_ref, fz_ref, slot, i, k):
    for n in range(12):
        fz_ref[n, i, window(k)] = weighted(
            *[tmp_ref[n, slot, ln.rows(ROWS * k + step)] for step in (0, 1, 2)]
        )


def filter_x(hz_ref, hu_ref, i, k):
    for comp in range(3):
        hu_ref[comp, i, window(k)] = 0.0625 * weighted(
            *[hz_ref[comp, i + step, window(k)] for step in (0, 1, 2)]
        )


def add_sums(ln, hu_ref, fz_ref, x, k, carry):
    numer, denom = carry
    at = 1 + ROWS * k
    mid = [hu_ref[comp, x + 1, ln.rows(at)] for comp in range(3)]
    slopes = [
        (
            hu_ref[comp, x + 2, ln.rows(at)] - hu_ref[comp, x, ln.rows(at)],
            ln.slope_y(mid[comp]),
            ln.slope_z(
                hu_ref[comp, x + 1, ln.rows(at + 1)], hu_ref[comp, x + 1, ln.rows(at - 1)]
            ),
        )
        for comp in range(3)
    ]
    rate, size = rates(slopes)
    size = 4.0 * size
    top, straight, crossed = [], [], []
    for n, (a, b) in enumerate(index_pairs):
        stress = weighted(*[fz_ref[n, x + step, window(k)] for step in (0, 1, 2)])
        product = weighted(*[fz_ref[6 + n, x + step, window(k)] for step in (0, 1, 2)])
        model = stress - size * rate[n]
        leonard = product - mid[a] * mid[b]
        top.append(leonard * model)
        (straight if a == b else crossed).append(model * model)
    numer = numer + ((top[0] + top[1]) + (top[2] + top[3]) + (top[4] + top[5]))
    denom = denom + (
        (straight[0] + straight[1] + straight[2])
        + 0.5 * (crossed[0] + crossed[1] + crossed[2])
    )
    return numer, denom


def strain_planes(ln, u_ref, mag_ref, tmp_ref, keep_ref, fz_ref, start, stop):
    windows = mag_ref.shape[1] // ROWS

    def plane(i):
        for k in range(1, windows):
            strain(ln, u_ref, mag_ref, tmp_ref, keep_ref, lax.rem(i, 2), i, k)

    def products(i):
        for k in range(1, windows - 1):
            filter_products(ln, tmp_ref, fz_ref, lax.rem(i, 2), i, k)

    def step(i, carry):
        products(i - 1)
        plane(i)
        return carry

    plane(start)
    lax.fori_loop(start + 1, stop, step, 0)
    products(stop - 1)


def sum_planes(ln, hu_ref, fz_ref, acc_ref, start, stop):
    def step(x, carry):
        for k in range(1, fz_ref.shape[2] // ROWS):
            carry = add_sums(ln, hu_ref, fz_ref, x, k, carry)
        return carry

    acc_ref[0], acc_ref[1] = lax.fori_loop(start, stop, step, (acc_ref[0], acc_ref[1]))


def interior_kernel(
    vel_ref, u_ref, keep_ref, fz_ref, hz_ref, hu_ref, mag_ref, acc_ref, tmp_ref
):
    nx = vel_ref.shape[1]
    windows = mag_ref.shape[1] // ROWS
    ln = Lanes(u_ref.shape[3])

    def fold(x, carry):
        for comp in range(3):
            store_plane(ln, u_ref, comp, WIDTH + x, vel_ref[comp, x])
        return carry

    lax.fori_loop(0, nx, fold, 0, unroll=2)

    def hat_z(x, carry):
        for k in range(1, windows):
            filter_z(ln, u_ref, hz_ref, WIDTH + x, k)
        return carry

    lax.fori_loop(0, nx, hat_z, 0)

    def hat_x(i, carry):
        for k in range(1, windows):
            filter_x(hz_ref, hu_ref, i, k)
        return carry

    lax.fori_loop(2, nx, hat_x, 0)
    strain_planes(ln, u_ref, mag_ref, tmp_ref, keep_ref, fz_ref, 2, nx)
    acc_ref[...] = jnp.zeros_like(acc_ref)
    sum_planes(ln, hu_ref, fz_ref, acc_ref, 2, nx - 2)


def fold_kernel(first_ref, second_ref, _, u_ref, edge_ref):
    planes = u_ref.shape[1]
    ln = Lanes(u_ref.shape[3])
    ordered = below_is_first("gx")
    for comp in range(3):
        for layer in range(WIDTH):
            first, second = first_ref[comp, layer], second_ref[comp, layer]
            below, above = jnp.where(ordered, first, second), jnp.where(ordered, second, first)
            store_plane(ln, u_ref, comp, layer, below)
            store_plane(ln, u_ref, comp, planes - WIDTH + layer, above)
    edges = []
    for comp in range(3):
        for slot in range(planes):
            edges.append((comp, slot))
    row = lax.broadcasted_iota(jnp.int32, (ROWS, edge_ref.shape[1]), 0)
    per_window = ROWS // WIDTH
    for at in range(0, len(edges), per_window):
        packed = None
        for n, (comp, slot) in enumerate(edges[at : at + per_window]):
            for layer in range(WIDTH):
                to = WIDTH * n + WIDTH - 1 - layer
                rows = u_ref[comp, slot, ln.rows(TOP + layer - to)]
                packed = rows if packed is None else jnp.where(row == to, rows, packed)
        edge_ref[window(at // per_window)] = packed


def sides_kernel(
    u_ref, _1, _2, _3, _4, _5, _6,
    keep_ref, fz_ref, hz_ref, hu_ref, mag_ref, acc_ref, tmp_ref,
):
    planes = u_ref.shape[1]
    nx = planes - 2 * WIDTH
    windows = mag_ref.shape[1] // ROWS
    ln = Lanes(u_ref.shape[3])
    for start, stop in ((0, WIDTH), (planes - WIDTH, planes)):
        for slot in range(start, stop):
            for k in range(1, windows):
                filter_z(ln, u_ref, hz_ref, slot, k)
    for start, stop in ((0, 2), (nx, nx + 2)):
        for i in range(start, stop):
            for k in range(1, windows):
                filter_x(hz_ref, hu_ref, i, k)
        strain_planes(ln, u_ref, mag_ref, tmp_ref, keep_ref, fz_ref, start, stop)
    sum_planes(ln, hu_ref, fz_ref, acc_ref, 0, 2)
    sum_planes(ln, hu_ref, fz_ref, acc_ref, nx - 2, nx)


def rim_kernel(
    first_ref, second_ref, _1, _2, _3, _4, acc_ref, u_ref, tmp_ref, hu_ref, mag_ref,
    plain_ref, sums_ref, turned, fz, hz,
):
    planes, _, lanes = u_ref.shape[1:]
    nx = planes - 2 * WIDTH
    ny = lanes // 2
    half = plain_ref.shape[2] // 2
    ln = Lanes(lanes)
    count = first_ref.shape[0]
    upper = lax.broadcasted_iota(jnp.int32, first_ref.shape, 1) >= ny
    take_first = jnp.logical_not(jnp.logical_xor(upper, below_is_first("gz")))
    turned[ROWS : ROWS + count] = pltpu.roll(
        jnp.where(take_first, first_ref[...], second_ref[...]), ny, 1
    )
    for comp in range(3):
        for slot in range(planes):
            at = WIDTH * (comp * planes + slot + 1)
            u_ref[comp, slot, ln.rows(TOP - ROWS)] = turned[ln.rows(at)]
    for slot in range(planes):
        filter_z(ln, u_ref, hz, slot, 0)
    for i in range(nx + 2):
        filter_x(hz, hu_ref, i, 0)
    for i in range(nx + 2):
        strain(ln, u_ref, mag_ref, tmp_ref, None, i, i, 0)
    for i in range(nx + 2):
        filter_products(ln, tmp_ref, fz, i, i, 0)
    carry = acc_ref[0], acc_ref[1]
    for x in range(nx):
        carry = add_sums(ln, hu_ref, fz, x, 0, carry)
    numer, denom = [jnp.sum(part, axis=0, keepdims=True) for part in carry]
    numer = numer + pltpu.roll(numer, ny, 1)
    denom = denom + pltpu.roll(denom, ny, 1)
    both = jnp.where(lax.broadcasted_iota(jnp.int32, (1, lanes), 1) < ny, numer, denom)
    sums_ref[...] = jnp.broadcast_to(both, sums_ref.shape)
    for x in range(nx):
        plain_ref[x] = from_folded(mag_ref[x + 1, ln.rows(1, half)])


def finish_kernel(cells, parts_ref, mag_ref, coefficient_ref, eddy_ref):
    lanes = parts_ref.shape[1]
    ny = lanes // 2
    sums = jnp.sum(parts_ref[...], axis=0, keepdims=True)
    numer = sums[:, :ny]
    denom = pltpu.roll(sums, ny, 1)[:, :ny]
    coefficient = numer / cells / (denom / cells + 1e-06)
    coefficient_ref[...] = coefficient
    column = jnp.broadcast_to(coefficient, (mag_ref.shape[2], ny)).T
    for x in range(mag_ref.shape[0]):
        eddy_ref[x] = column * mag_ref[x]


def call(
    kernel, name, shapes, operands, cycles, aliases=None, scratch=()
):
    return pl.pallas_call(
        kernel,
        out_shape=tuple(jax.ShapeDtypeStruct(shape, jnp.float32) for shape in shapes),
        in_specs=[VMEM] * len(operands),
        out_specs=tuple(VMEM for _ in shapes),
        scratch_shapes=[
            pltpu.VMEM(item, jnp.float32) if isinstance(item, tuple) else item for item in scratch
        ],
        input_output_aliases=aliases or {},
        compiler_params=pltpu.CompilerParams(vmem_limit_bytes=8 * 1024 * 1024),
        cost_estimate=pl.CostEstimate(
            flops=cycles * 4096, bytes_accessed=0, transcendentals=0
        ),
        name=name,
    )(*operands)


def on_device(velocity):
    nx, ny, nz = velocity.shape[1:]
    half, lanes = nz // 2, 2 * ny
    planes = nx + 2 * WIDTH
    tall, windowed = half + 3 * ROWS, half + ROWS
    u_shape = (3, planes, tall, lanes)
    work = (
        (12, nx + 2, 2 * ROWS, lanes),
        (12, nx + 2, half, lanes),
        (3, planes, windowed, lanes),
        (3, nx + 2, windowed, lanes),
        (nx + 2, windowed, lanes),
        (2, ROWS, lanes),
    )
    window_pair = ((12, 2, windowed, lanes),)
    low, high = velocity[:, :WIDTH], velocity[:, nx - WIDTH :]
    flag = first_goes_below("gx")
    first, second = jnp.where(flag, low, high), jnp.where(flag, high, low)
    first, second = swap_edges(first, second, "gx")
    u, *fields = call(
        interior_kernel, "interior", (u_shape, *work), (velocity,), 6000, scratch=window_pair
    )
    edge_shape = (3 * planes * WIDTH, lanes)
    u, edges = call(
        fold_kernel, "fold", (u_shape, edge_shape), (first, second, u), 800, {2: 0}
    )
    first, second = swap_edges(edges, edges, "gz")
    keep, _, _, hu, mag, acc = call(
        sides_kernel,
        "sides",
        work,
        (u, *fields),
        4000,
        {1 + n: n for n in range(6)},
        window_pair,
    )
    count = lax.axis_size("gx") * lax.axis_size("gz")
    *_, magnitude, sums = call(
        rim_kernel,
        "rim",
        (u_shape, work[0], work[3], work[4], (nx, ny, nz), (count, lanes)),
        (first, second, u, keep, hu, mag, acc),
        1000,
        {2 + n: n for n in range(4)},
        scratch=(
            (ROWS + edge_shape[0], lanes),
            (12, nx + 2, ROWS, lanes),
            (3, planes, ROWS, lanes),
        ),
    )
    parts = lax.all_to_all(sums, ("gx", "gz"), 0, 0, tiled=True)
    cells = nx * lax.axis_size("gx") * nz * lax.axis_size("gz")
    coefficient, eddy_viscosity = call(
        functools.partial(finish_kernel, cells),
        "finish",
        ((1, ny), (nx, ny, nz)),
        (parts, magnitude),
        500,
    )
    return (coefficient[0], eddy_viscosity)


def solution(mesh):
    in_specs = (P(None, "gx", None, "gz"),)
    out_specs = (P(), P("gx", None, "gz"))
    return jax.shard_map(
        on_device, mesh=mesh, in_specs=in_specs, out_specs=out_specs, check_vma=False
    )
```

```python
import functools

import jax
import jax.numpy as jnp
from jax import lax
from jax.experimental import pallas as pl
from jax.experimental.pallas import tpu as pltpu
from jax.sharding import PartitionSpec as P


WIDTH = 2
ROWS = 8
index_pairs = ((0, 0), (1, 1), (2, 2), (0, 1), (0, 2), (1, 2))
STRIP = 16
TOP = 9

VMEM = pl.BlockSpec(memory_space=pltpu.VMEM)


def swap_axes(axis):
    count = lax.axis_size(axis)
    if count % 2:
        forward = [(i, (i + 1) % count) for i in range(count)]
        return forward, [(target, source) for source, target in forward]
    far = [(i, (i + 1 if i % 2 else i - 1) % count) for i in range(count)]
    return [(i, i ^ 1) for i in range(count)], far


def below_is_first(axis):
    if lax.axis_size(axis) % 2:
        return True
    return lax.rem(lax.axis_index(axis), 2) == 1


def first_goes_below(axis):
    if lax.axis_size(axis) % 2:
        return False
    return below_is_first(axis)


def mirrored(plane):
    lanes = plane.shape[1]
    lane = lax.broadcasted_iota(jnp.int32, plane.shape, 1)
    return jnp.take_along_axis(plane, lanes - 1 - lane, axis=1)


def to_folded(plane, rows):
    return jnp.concatenate([plane[:, :rows], mirrored(plane)[:, :rows]], axis=0).T


def from_folded(folded):
    half, lanes = folded.shape
    ny = lanes // 2
    turned = folded.T
    both = jnp.concatenate([turned[:ny], turned[ny:]], axis=1)
    lane = lax.broadcasted_iota(jnp.int32, both.shape, 1)
    return jnp.take_along_axis(both, jnp.where(lane < half, lane, 3 * half - 1 - lane), axis=1)


class Lanes:
    def __init__(self, lanes):
        self.zero = jnp.minimum(lax.axis_index("gx"), 0)
        lane = lax.broadcasted_iota(jnp.int32, (ROWS, lanes), 1)
        row_y = lax.rem(lane, lanes // 2)
        self.first, self.last = row_y == 0, row_y == lanes // 2 - 1
        self.scale = jnp.where(self.first | self.last, 2.0, 1.0).astype(jnp.float32)
        self.sign = jnp.where(lane < lanes // 2, 1.0, -1.0).astype(jnp.float32)

    def rows(self, start, count=ROWS):
        return pl.ds(self.zero + start, count)

    def slope_y(self, field):
        lanes = field.shape[1]
        up = jnp.where(self.last, field, pltpu.roll(field, lanes - 1, 1))
        down = jnp.where(self.first, field, pltpu.roll(field, 1, 1))
        return (up - down) * self.scale

    def slope_z(self, after, before):
        return (after - before) * self.sign


def window(k):
    return pl.ds(ROWS * k, ROWS)


def store_plane(ln, u_ref, comp, slot, plane):
    count = plane.shape[1] // 2 + ROWS
    folded = to_folded(plane, count)
    for k in range(count // ROWS):
        u_ref[comp, slot, ln.rows(TOP + ROWS * k)] = folded[ROWS * k : ROWS * (k + 1)]


def rates(slopes):
    rate = [
        slopes[i][i] if i == j else slopes[i][j] + slopes[j][i] for i, j in index_pairs
    ]
    squares = [r * r for r in rate]
    straight = squares[0] + squares[1] + squares[2]
    crossed = squares[3] + squares[4] + squares[5]
    return rate, 0.5 * jnp.sqrt((straight + straight) + crossed)


def weighted(low, mid, high):
    return (low + high) + (mid + mid)


def filter_z(ln, u_ref, hz_ref, slot, k):
    at = ROWS * (k + 1)
    for comp in range(3):
        hz_ref[comp, slot, window(k)] = weighted(
            *[u_ref[comp, slot, ln.rows(at + step)] for step in (-1, 0, 1)]
        )


def strain(ln, u_ref, mag_ref, tmp_ref, keep_ref, slot, i, k):
    at = ROWS * (k + 1)
    mid = [u_ref[comp, i + 1, ln.rows(at)] for comp in range(3)]
    slopes = [
        (
            u_ref[comp, i + 2, ln.rows(at)] - u_ref[comp, i, ln.rows(at)],
            ln.slope_y(mid[comp]),
            ln.slope_z(u_ref[comp, i + 1, ln.rows(at + 1)], u_ref[comp, i + 1, ln.rows(at - 1)]),
        )
        for comp in range(3)
    ]
    rate, size = rates(slopes)
    mag_ref[i, window(k)] = size
    scaled = size * 0.0625
    quarter = [0.25 * m for m in mid]
    for n, (a, b) in enumerate(index_pairs):
        for at, value in ((n, scaled * rate[n]), (6 + n, quarter[a] * quarter[b])):
            tmp_ref[at, slot, window(k)] = value
            if k == 1:
                keep_ref[at, i, window(1)] = value


def filter_products(ln, tmp_ref, fz_ref, slot, i, k):
    for n in range(12):
        fz_ref[n, i, window(k)] = weighted(
            *[tmp_ref[n, slot, ln.rows(ROWS * k + step)] for step in (0, 1, 2)]
        )


def filter_x(hz_ref, hu_ref, i, k):
    for comp in range(3):
        hu_ref[comp, i, window(k)] = 0.0625 * weighted(
            *[hz_ref[comp, i + step, window(k)] for step in (0, 1, 2)]
        )


def add_sums(ln, hu_ref, fz_ref, x, k, carry):
    numer, denom = carry
    at = 1 + ROWS * k
    mid = [hu_ref[comp, x + 1, ln.rows(at)] for comp in range(3)]
    slopes = [
        (
            hu_ref[comp, x + 2, ln.rows(at)] - hu_ref[comp, x, ln.rows(at)],
            ln.slope_y(mid[comp]),
            ln.slope_z(
                hu_ref[comp, x + 1, ln.rows(at + 1)], hu_ref[comp, x + 1, ln.rows(at - 1)]
            ),
        )
        for comp in range(3)
    ]
    rate, size = rates(slopes)
    size = 4.0 * size
    top, straight, crossed = [], [], []
    for n, (a, b) in enumerate(index_pairs):
        stress = weighted(*[fz_ref[n, x + step, window(k)] for step in (0, 1, 2)])
        product = weighted(*[fz_ref[6 + n, x + step, window(k)] for step in (0, 1, 2)])
        model = stress - size * rate[n]
        leonard = product - mid[a] * mid[b]
        top.append(leonard * model)
        (straight if a == b else crossed).append(model * model)
    numer = numer + ((top[0] + top[1]) + (top[2] + top[3]) + (top[4] + top[5]))
    denom = denom + (
        (straight[0] + straight[1] + straight[2])
        + 0.5 * (crossed[0] + crossed[1] + crossed[2])
    )
    return numer, denom


def strain_planes(ln, u_ref, mag_ref, tmp_ref, keep_ref, fz_ref, start, stop):
    windows = mag_ref.shape[1] // ROWS

    def plane(i):
        for k in range(1, windows):
            strain(ln, u_ref, mag_ref, tmp_ref, keep_ref, lax.rem(i, 2), i, k)

    def products(i):
        for k in range(1, windows - 1):
            filter_products(ln, tmp_ref, fz_ref, lax.rem(i, 2), i, k)

    def step(i, carry):
        products(i - 1)
        plane(i)
        return carry

    plane(start)
    lax.fori_loop(start + 1, stop, step, 0)
    products(stop - 1)


def sum_planes(ln, hu_ref, fz_ref, acc_ref, start, stop):
    def step(x, carry):
        for k in range(1, fz_ref.shape[2] // ROWS):
            carry = add_sums(ln, hu_ref, fz_ref, x, k, carry)
        return carry

    acc_ref[0], acc_ref[1] = lax.fori_loop(start, stop, step, (acc_ref[0], acc_ref[1]))


def pack_edges(ln, u_ref, entries):
    packed = None
    for n, (comp, slot) in enumerate(entries):
        for layer in range(WIDTH):
            to = WIDTH * n + WIDTH - 1 - layer
            rows = u_ref[comp, slot, ln.rows(TOP + layer - to)]
            row = lax.broadcasted_iota(jnp.int32, rows.shape, 0)
            packed = rows if packed is None else jnp.where(row == to, rows, packed)
    return packed


def pack_all(ln, u_ref, entries, edge_ref, start):
    for at in range(0, len(entries), ROWS // WIDTH):
        to = start + WIDTH * at
        edge_ref[to : to + ROWS] = pack_edges(ln, u_ref, entries[at : at + ROWS // WIDTH])


def load_kernel(vel_ref, first_ref, second_ref, strip_ref, top_ref):
    nx = vel_ref.shape[1]
    ln = Lanes(strip_ref.shape[1])
    flag = first_goes_below("gx")
    entries = [(comp, layer) for comp in range(3) for layer in range(WIDTH)]
    for comp, layer in entries:
        low, high = vel_ref[comp, layer], vel_ref[comp, nx - WIDTH + layer]
        first_ref[comp, layer] = jnp.where(flag, low, high)
        second = jnp.where(flag, high, low)
        second_ref[comp, layer] = second
        top_ref[comp, layer, ln.rows(TOP)] = to_folded(second, ROWS)
    pack_all(ln, top_ref, entries, strip_ref, 0)


def near_slots(nx):
    flag = below_is_first("gx")
    return jnp.where(flag, 0, WIDTH), jnp.where(flag, nx + WIDTH, 0)


def fold_kernel(vel_ref, first_ref, strip_ref, u_ref, edge_ref):
    nx = vel_ref.shape[1]
    ln = Lanes(u_ref.shape[3])
    start, _ = near_slots(nx)
    first_slot = jnp.where(below_is_first("gx"), 0, nx + WIDTH)
    for layer in range(WIDTH):
        for comp in range(3):
            store_plane(ln, u_ref, comp, first_slot + layer, first_ref[comp, layer])

    def fold(x, carry):
        for comp in range(3):
            store_plane(ln, u_ref, comp, WIDTH + x, vel_ref[comp, x])
        return carry

    lax.fori_loop(0, nx, fold, 0, unroll=4)
    entries = [(comp, start + n) for comp in range(3) for n in range(nx + WIDTH)]
    count = strip_ref.shape[0]
    edge_ref[:count] = strip_ref[...]
    pack_all(ln, u_ref, entries, edge_ref, count)


def interior_kernel(
    u_ref, keep_ref, fz_ref, hz_ref, hu_ref, mag_ref, acc_ref, tmp_ref
):
    nx = u_ref.shape[1] - 2 * WIDTH
    windows = mag_ref.shape[1] // ROWS
    ln = Lanes(u_ref.shape[3])
    start, _ = near_slots(nx)

    def hat_z(slot, carry):
        for k in range(1, windows):
            filter_z(ln, u_ref, hz_ref, slot, k)
        return carry

    lax.fori_loop(start, start + nx + WIDTH, hat_z, 0)

    def hat_x(i, carry):
        for k in range(1, windows):
            filter_x(hz_ref, hu_ref, i, k)
        return carry

    lax.fori_loop(start, start + nx, hat_x, 0)
    strain_planes(ln, u_ref, mag_ref, tmp_ref, keep_ref, fz_ref, start, start + nx)
    acc_ref[...] = jnp.zeros_like(acc_ref)
    sum_planes(ln, hu_ref, fz_ref, acc_ref, start, start + nx - WIDTH)


def sides_kernel(
    second_ref, _0, _1, _2, _3, _4, _5, _6,
    u_ref, keep_ref, fz_ref, hz_ref, hu_ref, mag_ref, acc_ref, tmp_ref,
):
    nx = u_ref.shape[1] - 2 * WIDTH
    windows = mag_ref.shape[1] // ROWS
    ln = Lanes(u_ref.shape[3])
    _, slot = near_slots(nx)
    plane = jnp.where(below_is_first("gx"), nx, 0)
    inner = jnp.where(below_is_first("gx"), nx - WIDTH, 0)
    for layer in range(WIDTH):
        for comp in range(3):
            store_plane(ln, u_ref, comp, slot + layer, second_ref[comp, layer])
    for layer in range(WIDTH):
        for k in range(1, windows):
            filter_z(ln, u_ref, hz_ref, slot + layer, k)
    for layer in range(WIDTH):
        for k in range(1, windows):
            filter_x(hz_ref, hu_ref, plane + layer, k)
    strain_planes(ln, u_ref, mag_ref, tmp_ref, keep_ref, fz_ref, plane, plane + WIDTH)
    sum_planes(ln, hu_ref, fz_ref, acc_ref, inner, inner + WIDTH)


def rim_kernel(
    first_ref, second_ref, _1, _2, _3, _4, acc_ref, u_ref, tmp_ref, hu_ref, mag_ref,
    plain_ref, sums_ref, turned, fz, hz,
):
    planes, _, lanes = u_ref.shape[1:]
    nx = planes - 2 * WIDTH
    ny = lanes // 2
    half = plain_ref.shape[2] // 2
    ln = Lanes(lanes)
    count = first_ref.shape[0]
    upper = lax.broadcasted_iota(jnp.int32, first_ref.shape, 1) >= ny
    take_first = jnp.logical_not(jnp.logical_xor(upper, below_is_first("gz")))
    turned[ROWS : ROWS + count] = pltpu.roll(
        jnp.where(take_first, first_ref[...], second_ref[...]), ny, 1
    )
    start, far = near_slots(nx)
    places = [(comp, far + n) for comp in range(3) for n in range(WIDTH)]
    rest = [(comp, start + n) for comp in range(3) for n in range(nx + WIDTH)]
    for first_row, entries in ((0, places), (STRIP, rest)):
        for n, (comp, slot) in enumerate(entries):
            at = first_row + WIDTH * (n + 1)
            u_ref[comp, slot, ln.rows(TOP - ROWS)] = turned[ln.rows(at)]
    for slot in range(planes):
        filter_z(ln, u_ref, hz, slot, 0)
    for i in range(nx + 2):
        filter_x(hz, hu_ref, i, 0)
    for i in range(nx + 2):
        strain(ln, u_ref, mag_ref, tmp_ref, None, i, i, 0)
    for i in range(nx + 2):
        filter_products(ln, tmp_ref, fz, i, i, 0)
    carry = acc_ref[0], acc_ref[1]
    for x in range(nx):
        carry = add_sums(ln, hu_ref, fz, x, 0, carry)
    numer, denom = [jnp.sum(part, axis=0, keepdims=True) for part in carry]
    numer = numer + pltpu.roll(numer, ny, 1)
    denom = denom + pltpu.roll(denom, ny, 1)
    both = jnp.where(lax.broadcasted_iota(jnp.int32, (1, lanes), 1) < ny, numer, denom)
    sums_ref[...] = jnp.broadcast_to(both, sums_ref.shape)
    for x in range(nx):
        plain_ref[x] = from_folded(mag_ref[x + 1, ln.rows(1, half)])


def finish_kernel(cells, parts_ref, mag_ref, coefficient_ref, eddy_ref):
    lanes = parts_ref.shape[1]
    ny = lanes // 2
    sums = jnp.sum(parts_ref[...], axis=0, keepdims=True)
    numer = sums[:, :ny]
    denom = pltpu.roll(sums, ny, 1)[:, :ny]
    coefficient = numer / cells / (denom / cells + 1e-06)
    coefficient_ref[...] = coefficient
    column = jnp.broadcast_to(coefficient, (mag_ref.shape[2], ny)).T
    for x in range(mag_ref.shape[0]):
        eddy_ref[x] = column * mag_ref[x]


def call(kernel, shapes, operands, cycles, aliases=None, scratch=()):
    return pl.pallas_call(
        kernel,
        out_shape=tuple(jax.ShapeDtypeStruct(shape, jnp.float32) for shape in shapes),
        in_specs=[VMEM] * len(operands),
        out_specs=tuple(VMEM for _ in shapes),
        scratch_shapes=[
            pltpu.VMEM(item, jnp.float32) if isinstance(item, tuple) else item for item in scratch
        ],
        input_output_aliases=aliases or {},
        compiler_params=pltpu.CompilerParams(vmem_limit_bytes=8 * 1024 * 1024),
        cost_estimate=pl.CostEstimate(
            flops=cycles * 4096, bytes_accessed=0, transcendentals=0
        ),
    )(*operands)


def on_device(velocity):
    nx, ny, nz = velocity.shape[1:]
    half, lanes = nz // 2, 2 * ny
    planes = nx + 2 * WIDTH
    tall, windowed = half + 3 * ROWS, half + ROWS
    u_shape = (3, planes, tall, lanes)
    work = (
        (12, nx + 2, 2 * ROWS, lanes),
        (12, nx + 2, half, lanes),
        (3, planes, windowed, lanes),
        (3, nx + 2, windowed, lanes),
        (nx + 2, windowed, lanes),
        (2, ROWS, lanes),
    )
    window_pair = ((12, 2, windowed, lanes),)
    halo = (3, WIDTH, ny, nz)
    strip_shape = (STRIP, lanes)
    first, second, strip = call(
        load_kernel,
        (halo, halo, strip_shape),
        (velocity,),
        500,
        scratch=((3, WIDTH, 3 * ROWS, lanes),),
    )
    to_first, to_second = swap_axes("gx")
    strip = lax.ppermute(strip, "gx", to_second)
    first = lax.ppermute(first, "gx", to_first)
    second = lax.ppermute(second, "gx", to_second)
    edge_rows = STRIP + -(-3 * (nx + WIDTH) * WIDTH // ROWS) * ROWS
    u, edges = call(fold_kernel, (u_shape, (edge_rows, lanes)), (velocity, first, strip), 1500)
    to_first, to_second = swap_axes("gz")
    low = lax.ppermute(edges, "gz", to_second)
    high = lax.ppermute(edges, "gz", to_first)
    fields = call(interior_kernel, work, (u,), 6000, scratch=window_pair)
    u, keep, _, _, hu, mag, acc = call(
        sides_kernel,
        (u_shape, *work),
        (second, u, *fields),
        2000,
        {1 + n: n for n in range(7)},
        window_pair,
    )
    count = lax.axis_size("gx") * lax.axis_size("gz")
    *_, magnitude, sums = call(
        rim_kernel,
        (u_shape, work[0], work[3], work[4], (nx, ny, nz), (count, lanes)),
        (high, low, u, keep, hu, mag, acc),
        1000,
        {2 + n: n for n in range(4)},
        scratch=(
            (ROWS + edge_rows, lanes),
            (12, nx + 2, ROWS, lanes),
            (3, planes, ROWS, lanes),
        ),
    )
    parts = lax.all_to_all(sums, ("gx", "gz"), 0, 0, tiled=True)
    cells = nx * lax.axis_size("gx") * nz * lax.axis_size("gz")
    coefficient, eddy_viscosity = call(
        functools.partial(finish_kernel, cells), ((1, ny), (nx, ny, nz)), (parts, magnitude), 500
    )
    return (coefficient[0], eddy_viscosity)


def solution(mesh):
    in_specs = (P(None, "gx", None, "gz"),)
    out_specs = (P(), P("gx", None, "gz"))
    return jax.shard_map(
        on_device, mesh=mesh, in_specs=in_specs, out_specs=out_specs, check_vma=False
    )
```

```python
import functools

import jax
import jax.numpy as jnp
from jax import lax
from jax.experimental import pallas as pl
from jax.experimental.pallas import tpu as pltpu
from jax.sharding import PartitionSpec as P


WIDTH = 2
ROWS = 8
index_pairs = ((0, 0), (1, 1), (2, 2), (0, 1), (0, 2), (1, 2))
STRIP = 16
TOP = 9

VMEM = pl.BlockSpec(memory_space=pltpu.VMEM)


def swap_axes(axis):
    count = lax.axis_size(axis)
    if count % 2:
        forward = [(i, (i + 1) % count) for i in range(count)]
        return forward, [(target, source) for source, target in forward]
    far = [(i, (i + 1 if i % 2 else i - 1) % count) for i in range(count)]
    return [(i, i ^ 1) for i in range(count)], far


def below_is_first(axis):
    if lax.axis_size(axis) % 2:
        return True
    return lax.rem(lax.axis_index(axis), 2) == 1


def first_goes_below(axis):
    if lax.axis_size(axis) % 2:
        return False
    return below_is_first(axis)


def mirrored(plane):
    lanes = plane.shape[1]
    lane = lax.broadcasted_iota(jnp.int32, plane.shape, 1)
    return jnp.take_along_axis(plane, lanes - 1 - lane, axis=1)


def to_folded(plane, rows):
    return jnp.concatenate([plane[:, :rows], mirrored(plane)[:, :rows]], axis=0).T


def from_folded(folded):
    half, lanes = folded.shape
    ny = lanes // 2
    turned = folded.T
    both = jnp.concatenate([turned[:ny], turned[ny:]], axis=1)
    lane = lax.broadcasted_iota(jnp.int32, both.shape, 1)
    return jnp.take_along_axis(both, jnp.where(lane < half, lane, 3 * half - 1 - lane), axis=1)


class Lanes:
    def __init__(self, lanes):
        self.zero = jnp.minimum(lax.axis_index("gx"), 0)
        lane = lax.broadcasted_iota(jnp.int32, (ROWS, lanes), 1)
        row_y = lax.rem(lane, lanes // 2)
        self.first, self.last = row_y == 0, row_y == lanes // 2 - 1
        self.scale = jnp.where(self.first | self.last, 2.0, 1.0).astype(jnp.float32)
        self.sign = jnp.where(lane < lanes // 2, 1.0, -1.0).astype(jnp.float32)

    def rows(self, start, count=ROWS):
        return pl.ds(self.zero + start, count)

    def slope_y(self, field):
        lanes = field.shape[1]
        up = jnp.where(self.last, field, pltpu.roll(field, lanes - 1, 1))
        down = jnp.where(self.first, field, pltpu.roll(field, 1, 1))
        return (up - down) * self.scale

    def slope_z(self, after, before):
        return (after - before) * self.sign


def window(k):
    return pl.ds(ROWS * k, ROWS)


def store_plane(ln, u_ref, comp, slot, plane):
    count = plane.shape[1] // 2 + ROWS
    folded = to_folded(plane, count)
    for k in range(count // ROWS):
        u_ref[comp, slot, ln.rows(TOP + ROWS * k)] = folded[ROWS * k : ROWS * (k + 1)]


def rates(slopes):
    rate = [
        slopes[i][i] if i == j else slopes[i][j] + slopes[j][i] for i, j in index_pairs
    ]
    squares = [r * r for r in rate]
    straight = squares[0] + squares[1] + squares[2]
    crossed = squares[3] + squares[4] + squares[5]
    return rate, 0.5 * jnp.sqrt((straight + straight) + crossed)


def weighted(low, mid, high):
    return (low + high) + (mid + mid)


def filter_z(ln, u_ref, hz_ref, slot, k):
    at = ROWS * (k + 1)
    for comp in range(3):
        hz_ref[comp, slot, window(k)] = weighted(
            *[u_ref[comp, slot, ln.rows(at + step)] for step in (-1, 0, 1)]
        )


def strain(ln, u_ref, mag_ref, tmp_ref, keep_ref, slot, i, k):
    at = ROWS * (k + 1)
    mid = [u_ref[comp, i + 1, ln.rows(at)] for comp in range(3)]
    slopes = [
        (
            u_ref[comp, i + 2, ln.rows(at)] - u_ref[comp, i, ln.rows(at)],
            ln.slope_y(mid[comp]),
            ln.slope_z(u_ref[comp, i + 1, ln.rows(at + 1)], u_ref[comp, i + 1, ln.rows(at - 1)]),
        )
        for comp in range(3)
    ]
    rate, size = rates(slopes)
    mag_ref[i, window(k)] = size
    scaled = size * 0.0625
    quarter = [0.25 * m for m in mid]
    for n, (a, b) in enumerate(index_pairs):
        for at, value in ((n, scaled * rate[n]), (6 + n, quarter[a] * quarter[b])):
            tmp_ref[at, slot, window(k)] = value
            if k == 1:
                keep_ref[at, i, window(1)] = value


def outer_size(ln, u_ref, mag_ref, i):
    at = TOP + 1
    slopes = [
        (
            u_ref[comp, i + 2, ln.rows(at)] - u_ref[comp, i, ln.rows(at)],
            ln.slope_y(u_ref[comp, i + 1, ln.rows(at)]),
            ln.slope_z(u_ref[comp, i + 1, ln.rows(at + 1)], u_ref[comp, i + 1, ln.rows(at - 1)]),
        )
        for comp in range(3)
    ]
    mag_ref[i, ln.rows(2)] = rates(slopes)[1]


def unfold_planes(ln, mag_ref, plain_ref, start, count):
    half = plain_ref.shape[2] // 2
    for n in range(count):
        plain_ref[start + n] = from_folded(mag_ref[start + n + 1, ln.rows(1, half)])


def filter_products(ln, tmp_ref, fz_ref, slot, i, k):
    for n in range(12):
        fz_ref[n, i, window(k)] = weighted(
            *[tmp_ref[n, slot, ln.rows(ROWS * k + step)] for step in (0, 1, 2)]
        )


def filter_x(hz_ref, hu_ref, i, k):
    for comp in range(3):
        hu_ref[comp, i, window(k)] = 0.0625 * weighted(
            *[hz_ref[comp, i + step, window(k)] for step in (0, 1, 2)]
        )


def add_sums(ln, hu_ref, fz_ref, x, k, carry):
    numer, denom = carry
    at = 1 + ROWS * k
    mid = [hu_ref[comp, x + 1, ln.rows(at)] for comp in range(3)]
    slopes = [
        (
            hu_ref[comp, x + 2, ln.rows(at)] - hu_ref[comp, x, ln.rows(at)],
            ln.slope_y(mid[comp]),
            ln.slope_z(
                hu_ref[comp, x + 1, ln.rows(at + 1)], hu_ref[comp, x + 1, ln.rows(at - 1)]
            ),
        )
        for comp in range(3)
    ]
    rate, size = rates(slopes)
    size = 4.0 * size
    top, straight, crossed = [], [], []
    for n, (a, b) in enumerate(index_pairs):
        stress = weighted(*[fz_ref[n, x + step, window(k)] for step in (0, 1, 2)])
        product = weighted(*[fz_ref[6 + n, x + step, window(k)] for step in (0, 1, 2)])
        model = stress - size * rate[n]
        leonard = product - mid[a] * mid[b]
        top.append(leonard * model)
        (straight if a == b else crossed).append(model * model)
    numer = numer + ((top[0] + top[1]) + (top[2] + top[3]) + (top[4] + top[5]))
    denom = denom + (
        (straight[0] + straight[1] + straight[2])
        + 0.5 * (crossed[0] + crossed[1] + crossed[2])
    )
    return numer, denom


def strain_planes(ln, u_ref, mag_ref, tmp_ref, keep_ref, fz_ref, start, stop):
    windows = mag_ref.shape[1] // ROWS

    def plane(i):
        for k in range(1, windows):
            strain(ln, u_ref, mag_ref, tmp_ref, keep_ref, lax.rem(i, 2), i, k)

    def products(i):
        for k in range(1, windows - 1):
            filter_products(ln, tmp_ref, fz_ref, lax.rem(i, 2), i, k)

    def step(i, carry):
        products(i - 1)
        plane(i)
        return carry

    plane(start)
    lax.fori_loop(start + 1, stop, step, 0)
    products(stop - 1)


def sum_planes(ln, hu_ref, fz_ref, acc_ref, start, stop):
    def step(x, carry):
        for k in range(1, fz_ref.shape[2] // ROWS):
            carry = add_sums(ln, hu_ref, fz_ref, x, k, carry)
        return carry

    acc_ref[0], acc_ref[1] = lax.fori_loop(start, stop, step, (acc_ref[0], acc_ref[1]))


def pack_edges(ln, u_ref, entries):
    packed = None
    for n, (comp, slot) in enumerate(entries):
        for layer in range(WIDTH):
            to = WIDTH * n + WIDTH - 1 - layer
            rows = u_ref[comp, slot, ln.rows(TOP + layer - to)]
            row = lax.broadcasted_iota(jnp.int32, rows.shape, 0)
            packed = rows if packed is None else jnp.where(row == to, rows, packed)
    return packed


def pack_all(ln, u_ref, entries, edge_ref, start):
    for at in range(0, len(entries), ROWS // WIDTH):
        to = start + WIDTH * at
        edge_ref[to : to + ROWS] = pack_edges(ln, u_ref, entries[at : at + ROWS // WIDTH])


def load_kernel(vel_ref, first_ref, second_ref, strip_ref, top_ref):
    nx = vel_ref.shape[1]
    ln = Lanes(strip_ref.shape[1])
    flag = first_goes_below("gx")
    entries = [(comp, layer) for comp in range(3) for layer in range(WIDTH)]
    for comp, layer in entries:
        low, high = vel_ref[comp, layer], vel_ref[comp, nx - WIDTH + layer]
        first_ref[comp, layer] = jnp.where(flag, low, high)
        second = jnp.where(flag, high, low)
        second_ref[comp, layer] = second
        top_ref[comp, layer, ln.rows(TOP)] = to_folded(second, ROWS)
    pack_all(ln, top_ref, entries, strip_ref, 0)


def near_slots(nx):
    flag = below_is_first("gx")
    return jnp.where(flag, 0, WIDTH), jnp.where(flag, nx + WIDTH, 0)


def edge_places(nx):
    start, far = near_slots(nx)
    near = jnp.where(below_is_first("gx"), start, nx + WIDTH)
    block = [(comp, WIDTH + x) for comp in range(3) for x in range(nx)]
    halos = [
        [(comp, slot + layer) for comp in range(3) for layer in range(WIDTH)]
        for slot in (far, near)
    ]
    return ((0, halos[0]), (STRIP, block), (STRIP + WIDTH * len(block), halos[1]))


def fold_kernel(vel_ref, u_ref, edge_ref):
    nx = vel_ref.shape[1]
    ln = Lanes(u_ref.shape[3])

    def fold(x, carry):
        for comp in range(3):
            store_plane(ln, u_ref, comp, WIDTH + x, vel_ref[comp, x])
        return carry

    lax.fori_loop(0, nx, fold, 0, unroll=4)
    row, entries = edge_places(nx)[1]
    pack_all(ln, u_ref, entries, edge_ref, row)


def near_kernel(first_ref, _0, _1, u_ref, edge_ref):
    nx = u_ref.shape[1] - 2 * WIDTH
    ln = Lanes(u_ref.shape[3])
    row, entries = edge_places(nx)[2]
    for n, (comp, slot) in enumerate(entries):
        store_plane(ln, u_ref, comp, slot, first_ref[comp, n % WIDTH])
    pack_all(ln, u_ref, entries, edge_ref, row)


def edge_kernel(strip_ref, _, edge_ref):
    edge_ref[:STRIP] = strip_ref[...]


def interior_kernel(
    u_ref, keep_ref, fz_ref, hz_ref, hu_ref, mag_ref, acc_ref, plain_ref, tmp_ref
):
    nx = u_ref.shape[1] - 2 * WIDTH
    windows = mag_ref.shape[1] // ROWS
    ln = Lanes(u_ref.shape[3])
    start, _ = near_slots(nx)

    def hat_z(slot, carry):
        for k in range(1, windows):
            filter_z(ln, u_ref, hz_ref, slot, k)
        return carry

    lax.fori_loop(start, start + nx + WIDTH, hat_z, 0)

    def hat_x(i, carry):
        for k in range(1, windows):
            filter_x(hz_ref, hu_ref, i, k)
        return carry

    lax.fori_loop(start, start + nx, hat_x, 0)
    strain_planes(ln, u_ref, mag_ref, tmp_ref, keep_ref, fz_ref, start, start + nx)
    acc_ref[...] = jnp.zeros_like(acc_ref)
    sum_planes(ln, hu_ref, fz_ref, acc_ref, start, start + nx - WIDTH)
    inner = jnp.maximum(start - 1, 0)
    for n in range(nx - 1):
        outer_size(ln, u_ref, mag_ref, inner + n + 1)
    unfold_planes(ln, mag_ref, plain_ref, inner, nx - 1)


def sides_kernel(
    second_ref, _0, _1, _2, _3, _4, _5, _6,
    u_ref, keep_ref, fz_ref, hz_ref, hu_ref, mag_ref, acc_ref, tmp_ref,
):
    nx = u_ref.shape[1] - 2 * WIDTH
    windows = mag_ref.shape[1] // ROWS
    ln = Lanes(u_ref.shape[3])
    _, slot = near_slots(nx)
    plane = jnp.where(below_is_first("gx"), nx, 0)
    inner = jnp.where(below_is_first("gx"), nx - WIDTH, 0)
    for layer in range(WIDTH):
        for comp in range(3):
            store_plane(ln, u_ref, comp, slot + layer, second_ref[comp, layer])
    for layer in range(WIDTH):
        for k in range(1, windows):
            filter_z(ln, u_ref, hz_ref, slot + layer, k)
    for layer in range(WIDTH):
        for k in range(1, windows):
            filter_x(hz_ref, hu_ref, plane + layer, k)
    strain_planes(ln, u_ref, mag_ref, tmp_ref, keep_ref, fz_ref, plane, plane + WIDTH)
    sum_planes(ln, hu_ref, fz_ref, acc_ref, inner, inner + WIDTH)


def rim_kernel(
    first_ref, second_ref, _1, _2, _3, _4, _5, acc_ref, u_ref, tmp_ref, hu_ref, mag_ref,
    plain_ref, outer_ref, sums_ref, turned, fz, hz,
):
    planes, _, lanes = u_ref.shape[1:]
    nx = planes - 2 * WIDTH
    ny = lanes // 2
    ln = Lanes(lanes)
    count = first_ref.shape[0]
    upper = lax.broadcasted_iota(jnp.int32, first_ref.shape, 1) >= ny
    take_first = jnp.logical_not(jnp.logical_xor(upper, below_is_first("gz")))
    turned[ROWS : ROWS + count] = pltpu.roll(
        jnp.where(take_first, first_ref[...], second_ref[...]), ny, 1
    )
    for first_row, entries in edge_places(nx):
        for n, (comp, slot) in enumerate(entries):
            at = first_row + WIDTH * (n + 1)
            u_ref[comp, slot, ln.rows(TOP - ROWS)] = turned[ln.rows(at)]
    for slot in range(planes):
        filter_z(ln, u_ref, hz, slot, 0)
    for i in range(nx + 2):
        filter_x(hz, hu_ref, i, 0)
    for i in range(nx + 2):
        strain(ln, u_ref, mag_ref, tmp_ref, None, i, i, 0)
    for i in range(nx + 2):
        filter_products(ln, tmp_ref, fz, i, i, 0)
    carry = acc_ref[0], acc_ref[1]
    for x in range(nx):
        carry = add_sums(ln, hu_ref, fz, x, 0, carry)
    numer, denom = [jnp.sum(part, axis=0, keepdims=True) for part in carry]
    numer = numer + pltpu.roll(numer, ny, 1)
    denom = denom + pltpu.roll(denom, ny, 1)
    both = jnp.where(lax.broadcasted_iota(jnp.int32, (1, lanes), 1) < ny, numer, denom)
    sums_ref[...] = jnp.broadcast_to(both, sums_ref.shape)
    for x in range(nx):
        outer_ref[x : x + 1] = mag_ref[x + 1, 1:2]
    unfold_planes(ln, mag_ref, plain_ref, jnp.where(below_is_first("gx"), nx - 1, 0), 1)


def finish_kernel(cells, parts_ref, mag_ref, outer_ref, coefficient_ref, eddy_ref):
    lanes = parts_ref.shape[1]
    ny = lanes // 2
    sums = jnp.sum(parts_ref[...], axis=0, keepdims=True)
    numer = sums[:, :ny]
    denom = pltpu.roll(sums, ny, 1)[:, :ny]
    coefficient = numer / cells / (denom / cells + 1e-06)
    coefficient_ref[...] = coefficient
    column = jnp.broadcast_to(coefficient, (mag_ref.shape[2], ny)).T
    outer = outer_ref[...].T
    lane = lax.broadcasted_iota(jnp.int32, column.shape, 1)
    for x in range(mag_ref.shape[0]):
        low, high = outer[:ny, x : x + 1], outer[ny:, x : x + 1]
        plane = jnp.where(lane == 0, low, mag_ref[x])
        eddy_ref[x] = column * jnp.where(lane == lane.shape[1] - 1, high, plane)


def call(kernel, shapes, operands, cycles, aliases=None, scratch=()):
    return pl.pallas_call(
        kernel,
        out_shape=tuple(jax.ShapeDtypeStruct(shape, jnp.float32) for shape in shapes),
        in_specs=[VMEM] * len(operands),
        out_specs=tuple(VMEM for _ in shapes),
        scratch_shapes=[
            pltpu.VMEM(item, jnp.float32) if isinstance(item, tuple) else item for item in scratch
        ],
        input_output_aliases=aliases or {},
        compiler_params=pltpu.CompilerParams(vmem_limit_bytes=8 * 1024 * 1024),
        cost_estimate=pl.CostEstimate(
            flops=cycles * 4096, bytes_accessed=0, transcendentals=0
        ),
    )(*operands)


def on_device(velocity):
    nx, ny, nz = velocity.shape[1:]
    half, lanes = nz // 2, 2 * ny
    planes = nx + 2 * WIDTH
    tall, windowed = half + 3 * ROWS, half + ROWS
    u_shape = (3, planes, tall, lanes)
    work = (
        (12, nx + 2, 2 * ROWS, lanes),
        (12, nx + 2, half, lanes),
        (3, planes, windowed, lanes),
        (3, nx + 2, windowed, lanes),
        (nx + 2, windowed, lanes),
        (2, ROWS, lanes),
    )
    window_pair = ((12, 2, windowed, lanes),)
    halo = (3, WIDTH, ny, nz)
    strip_shape = (STRIP, lanes)
    first, second, strip = call(
        load_kernel,
        (halo, halo, strip_shape),
        (velocity,),
        500,
        scratch=((3, WIDTH, 3 * ROWS, lanes),),
    )
    to_first, to_second = swap_axes("gx")
    strip = lax.ppermute(strip, "gx", to_second)
    first = lax.ppermute(first, "gx", to_first)
    second = lax.ppermute(second, "gx", to_second)
    edge_rows = STRIP + WIDTH * 3 * nx + STRIP
    edge_shape = (edge_rows, lanes)
    u, edges = call(fold_kernel, (u_shape, edge_shape), (velocity,), 1200)
    u, edges = call(near_kernel, (u_shape, edge_shape), (first, u, edges), 400, {1: 0, 2: 1})
    (edges,) = call(edge_kernel, (edge_shape,), (strip, edges), 50, {1: 0})
    to_first, to_second = swap_axes("gz")
    low = lax.ppermute(edges, "gz", to_second)
    high = lax.ppermute(edges, "gz", to_first)
    *fields, plain = call(interior_kernel, (*work, (nx, ny, nz)), (u,), 6000, scratch=window_pair)
    u, keep, _, _, hu, mag, acc = call(
        sides_kernel,
        (u_shape, *work),
        (second, u, *fields),
        2000,
        {1 + n: n for n in range(7)},
        window_pair,
    )
    count = lax.axis_size("gx") * lax.axis_size("gz")
    *_, plain, outer, sums = call(
        rim_kernel,
        (u_shape, work[0], work[3], work[4], (nx, ny, nz), (nx, lanes), (count, lanes)),
        (high, low, u, keep, hu, mag, plain, acc),
        1000,
        {2 + n: n for n in range(5)},
        scratch=(
            (ROWS + edge_rows, lanes),
            (12, nx + 2, ROWS, lanes),
            (3, planes, ROWS, lanes),
        ),
    )
    parts = lax.all_to_all(sums, ("gx", "gz"), 0, 0, tiled=True)
    cells = nx * lax.axis_size("gx") * nz * lax.axis_size("gz")
    coefficient, eddy_viscosity = call(
        functools.partial(finish_kernel, cells), ((1, ny), (nx, ny, nz)), (parts, plain, outer), 500
    )
    return (coefficient[0], eddy_viscosity)


def solution(mesh):
    in_specs = (P(None, "gx", None, "gz"),)
    out_specs = (P(), P("gx", None, "gz"))
    return jax.shard_map(
        on_device, mesh=mesh, in_specs=in_specs, out_specs=out_specs, check_vma=False
    )
```

```python
import functools

import jax
import jax.numpy as jnp
from jax import lax
from jax.experimental import pallas as pl
from jax.experimental.pallas import tpu as pltpu
from jax.sharding import PartitionSpec as P


WIDTH = 2
ROWS = 8
index_pairs = ((0, 0), (1, 1), (2, 2), (0, 1), (0, 2), (1, 2))
STRIP = 16
TOP = 9

VMEM = pl.BlockSpec(memory_space=pltpu.VMEM)


def swap_axes(axis):
    count = lax.axis_size(axis)
    if count % 2:
        forward = [(i, (i + 1) % count) for i in range(count)]
        return forward, [(target, source) for source, target in forward]
    far = [(i, (i + 1 if i % 2 else i - 1) % count) for i in range(count)]
    return [(i, i ^ 1) for i in range(count)], far


def below_is_first(axis):
    if lax.axis_size(axis) % 2:
        return True
    return lax.rem(lax.axis_index(axis), 2) == 1


def first_goes_below(axis):
    if lax.axis_size(axis) % 2:
        return False
    return below_is_first(axis)


def mirrored(plane):
    lanes = plane.shape[1]
    lane = lax.broadcasted_iota(jnp.int32, plane.shape, 1)
    return jnp.take_along_axis(plane, lanes - 1 - lane, axis=1)


def to_folded(plane, rows):
    return jnp.concatenate([plane[:, :rows], mirrored(plane)[:, :rows]], axis=0).T


def from_folded(folded):
    half, lanes = folded.shape
    ny = lanes // 2
    turned = folded.T
    both = jnp.concatenate([turned[:ny], turned[ny:]], axis=1)
    lane = lax.broadcasted_iota(jnp.int32, both.shape, 1)
    return jnp.take_along_axis(both, jnp.where(lane < half, lane, 3 * half - 1 - lane), axis=1)


class Lanes:
    def __init__(self, lanes):
        self.zero = jnp.minimum(lax.axis_index("gx"), 0)
        lane = lax.broadcasted_iota(jnp.int32, (ROWS, lanes), 1)
        row_y = lax.rem(lane, lanes // 2)
        self.first, self.last = row_y == 0, row_y == lanes // 2 - 1
        self.scale = jnp.where(self.first | self.last, 2.0, 1.0).astype(jnp.float32)
        self.sign = jnp.where(lane < lanes // 2, 1.0, -1.0).astype(jnp.float32)

    def rows(self, start, count=ROWS):
        return pl.ds(self.zero + start, count)

    def slope_y(self, field):
        lanes = field.shape[1]
        up = jnp.where(self.last, field, pltpu.roll(field, lanes - 1, 1))
        down = jnp.where(self.first, field, pltpu.roll(field, 1, 1))
        return (up - down) * self.scale

    def slope_z(self, after, before):
        return (after - before) * self.sign


def window(k):
    return pl.ds(ROWS * k, ROWS)


def store_plane(ln, u_ref, comp, slot, plane):
    count = plane.shape[1] // 2 + ROWS
    folded = to_folded(plane, count)
    for k in range(count // ROWS):
        u_ref[comp, slot, ln.rows(TOP + ROWS * k)] = folded[ROWS * k : ROWS * (k + 1)]


def rates(slopes):
    rate = [
        slopes[i][i] if i == j else slopes[i][j] + slopes[j][i] for i, j in index_pairs
    ]
    squares = [r * r for r in rate]
    straight = squares[0] + squares[1] + squares[2]
    crossed = squares[3] + squares[4] + squares[5]
    return rate, 0.5 * jnp.sqrt((straight + straight) + crossed)


def weighted(low, mid, high):
    return (low + high) + (mid + mid)


def filter_z(ln, u_ref, hz_ref, slot, k):
    at = ROWS * (k + 1)
    for comp in range(3):
        hz_ref[comp, slot, window(k)] = weighted(
            *[u_ref[comp, slot, ln.rows(at + step)] for step in (-1, 0, 1)]
        )


def strain(ln, u_ref, mag_ref, tmp_ref, keep_ref, slot, i, k):
    at = ROWS * (k + 1)
    mid = [u_ref[comp, i + 1, ln.rows(at)] for comp in range(3)]
    slopes = [
        (
            u_ref[comp, i + 2, ln.rows(at)] - u_ref[comp, i, ln.rows(at)],
            ln.slope_y(mid[comp]),
            ln.slope_z(u_ref[comp, i + 1, ln.rows(at + 1)], u_ref[comp, i + 1, ln.rows(at - 1)]),
        )
        for comp in range(3)
    ]
    rate, size = rates(slopes)
    mag_ref[i, window(k)] = size
    scaled = size * 0.0625
    quarter = [0.25 * m for m in mid]
    for n, (a, b) in enumerate(index_pairs):
        for at, value in ((n, scaled * rate[n]), (6 + n, quarter[a] * quarter[b])):
            tmp_ref[at, slot, window(k)] = value
            if k == 1:
                keep_ref[at, i, window(1)] = value


def outer_size(ln, u_ref, mag_ref, i):
    at = TOP + 1
    slopes = [
        (
            u_ref[comp, i + 2, ln.rows(at)] - u_ref[comp, i, ln.rows(at)],
            ln.slope_y(u_ref[comp, i + 1, ln.rows(at)]),
            ln.slope_z(u_ref[comp, i + 1, ln.rows(at + 1)], u_ref[comp, i + 1, ln.rows(at - 1)]),
        )
        for comp in range(3)
    ]
    mag_ref[i, ln.rows(2)] = rates(slopes)[1]


def unfold_planes(ln, mag_ref, plain_ref, start, count):
    half = plain_ref.shape[2] // 2
    for n in range(count):
        plain_ref[start + n] = from_folded(mag_ref[start + n + 1, ln.rows(1, half)])


def filter_products(ln, tmp_ref, fz_ref, slot, i, k):
    for n in range(12):
        fz_ref[n, i, window(k)] = weighted(
            *[tmp_ref[n, slot, ln.rows(ROWS * k + step)] for step in (0, 1, 2)]
        )


def filter_x(hz_ref, hu_ref, i, k):
    for comp in range(3):
        hu_ref[comp, i, window(k)] = 0.0625 * weighted(
            *[hz_ref[comp, i + step, window(k)] for step in (0, 1, 2)]
        )


def add_sums(ln, hu_ref, fz_ref, x, k, carry):
    numer, denom = carry
    at = 1 + ROWS * k
    mid = [hu_ref[comp, x + 1, ln.rows(at)] for comp in range(3)]
    slopes = [
        (
            hu_ref[comp, x + 2, ln.rows(at)] - hu_ref[comp, x, ln.rows(at)],
            ln.slope_y(mid[comp]),
            ln.slope_z(
                hu_ref[comp, x + 1, ln.rows(at + 1)], hu_ref[comp, x + 1, ln.rows(at - 1)]
            ),
        )
        for comp in range(3)
    ]
    rate, size = rates(slopes)
    size = 4.0 * size
    top, straight, crossed = [], [], []
    for n, (a, b) in enumerate(index_pairs):
        stress = weighted(*[fz_ref[n, x + step, window(k)] for step in (0, 1, 2)])
        product = weighted(*[fz_ref[6 + n, x + step, window(k)] for step in (0, 1, 2)])
        model = stress - size * rate[n]
        leonard = product - mid[a] * mid[b]
        top.append(leonard * model)
        (straight if a == b else crossed).append(model * model)
    numer = numer + ((top[0] + top[1]) + (top[2] + top[3]) + (top[4] + top[5]))
    denom = denom + (
        (straight[0] + straight[1] + straight[2])
        + 0.5 * (crossed[0] + crossed[1] + crossed[2])
    )
    return numer, denom


def strain_planes(
    ln, u_ref, mag_ref, tmp_ref, keep_ref, fz_ref, start, stop, with_outer=False
):
    windows = mag_ref.shape[1] // ROWS

    def plane(i):
        if with_outer:
            outer_size(ln, u_ref, mag_ref, i)
        for k in range(1, windows):
            strain(ln, u_ref, mag_ref, tmp_ref, keep_ref, lax.rem(i, 2), i, k)

    def products(i):
        for k in range(1, windows - 1):
            filter_products(ln, tmp_ref, fz_ref, lax.rem(i, 2), i, k)

    def step(i, carry):
        products(i - 1)
        plane(i)
        return carry

    plane(start)
    lax.fori_loop(start + 1, stop, step, 0)
    products(stop - 1)


def sum_planes(ln, hu_ref, fz_ref, acc_ref, start, stop, beside=None):
    def step(x, carry):
        if beside is not None:
            beside(x)
        for k in range(1, fz_ref.shape[2] // ROWS):
            carry = add_sums(ln, hu_ref, fz_ref, x, k, carry)
        return carry

    acc_ref[0], acc_ref[1] = lax.fori_loop(start, stop, step, (acc_ref[0], acc_ref[1]))


def pack_edges(ln, u_ref, entries):
    packed = None
    for n, (comp, slot) in enumerate(entries):
        for layer in range(WIDTH):
            to = WIDTH * n + WIDTH - 1 - layer
            rows = u_ref[comp, slot, ln.rows(TOP + layer - to)]
            row = lax.broadcasted_iota(jnp.int32, rows.shape, 0)
            packed = rows if packed is None else jnp.where(row == to, rows, packed)
    return packed


def pack_all(ln, u_ref, entries, edge_ref, start):
    for at in range(0, len(entries), ROWS // WIDTH):
        to = start + WIDTH * at
        edge_ref[to : to + ROWS] = pack_edges(ln, u_ref, entries[at : at + ROWS // WIDTH])


def load_kernel(vel_ref, first_ref, second_ref, strip_ref, top_ref):
    nx = vel_ref.shape[1]
    ln = Lanes(strip_ref.shape[1])
    flag = first_goes_below("gx")
    entries = [(comp, layer) for comp in range(3) for layer in range(WIDTH)]
    for comp, layer in entries:
        low, high = vel_ref[comp, layer], vel_ref[comp, nx - WIDTH + layer]
        first_ref[comp, layer] = jnp.where(flag, low, high)
        second = jnp.where(flag, high, low)
        second_ref[comp, layer] = second
        top_ref[comp, layer, ln.rows(TOP)] = to_folded(second, ROWS)
    pack_all(ln, top_ref, entries, strip_ref, 0)


def near_slots(nx):
    flag = below_is_first("gx")
    return jnp.where(flag, 0, WIDTH), jnp.where(flag, nx + WIDTH, 0)


def edge_places(nx):
    start, far = near_slots(nx)
    near = jnp.where(below_is_first("gx"), start, nx + WIDTH)
    block = [(comp, WIDTH + x) for comp in range(3) for x in range(nx)]
    halos = [
        [(comp, slot + layer) for comp in range(3) for layer in range(WIDTH)]
        for slot in (far, near)
    ]
    return ((0, halos[0]), (STRIP, block), (STRIP + WIDTH * len(block), halos[1]))


def fold_kernel(vel_ref, u_ref, edge_ref):
    nx = vel_ref.shape[1]
    ln = Lanes(u_ref.shape[3])

    def fold(x, carry):
        for comp in range(3):
            store_plane(ln, u_ref, comp, WIDTH + x, vel_ref[comp, x])
        return carry

    lax.fori_loop(0, nx, fold, 0, unroll=4)
    row, entries = edge_places(nx)[1]
    pack_all(ln, u_ref, entries, edge_ref, row)


def near_kernel(first_ref, _0, _1, u_ref, edge_ref):
    nx = u_ref.shape[1] - 2 * WIDTH
    ln = Lanes(u_ref.shape[3])
    row, entries = edge_places(nx)[2]
    for n, (comp, slot) in enumerate(entries):
        store_plane(ln, u_ref, comp, slot, first_ref[comp, n % WIDTH])
    pack_all(ln, u_ref, entries, edge_ref, row)


def edge_kernel(strip_ref, _, edge_ref):
    edge_ref[:STRIP] = strip_ref[...]


def interior_kernel(
    u_ref, keep_ref, fz_ref, hz_ref, hu_ref, mag_ref, acc_ref, plain_ref, tmp_ref
):
    nx = u_ref.shape[1] - 2 * WIDTH
    windows = mag_ref.shape[1] // ROWS
    ln = Lanes(u_ref.shape[3])
    start, _ = near_slots(nx)

    def hat_z(slot, carry):
        for k in range(1, windows):
            filter_z(ln, u_ref, hz_ref, slot, k)
        return carry

    lax.fori_loop(start, start + nx + WIDTH, hat_z, 0)

    def hat_x(i, carry):
        for k in range(1, windows):
            filter_x(hz_ref, hu_ref, i, k)
        return carry

    lax.fori_loop(start, start + nx, hat_x, 0)
    strain_planes(ln, u_ref, mag_ref, tmp_ref, keep_ref, fz_ref, start, start + nx, True)
    acc_ref[...] = jnp.zeros_like(acc_ref)
    inner = jnp.maximum(start - 1, 0)

    def unfold(x):
        unfold_planes(ln, mag_ref, plain_ref, inner + x - start, 1)

    sum_planes(ln, hu_ref, fz_ref, acc_ref, start, start + nx - WIDTH, unfold)
    unfold_planes(ln, mag_ref, plain_ref, inner + nx - WIDTH, 1)


def sides_kernel(
    second_ref, _0, _1, _2, _3, _4, _5, _6,
    u_ref, keep_ref, fz_ref, hz_ref, hu_ref, mag_ref, acc_ref, tmp_ref,
):
    nx = u_ref.shape[1] - 2 * WIDTH
    windows = mag_ref.shape[1] // ROWS
    ln = Lanes(u_ref.shape[3])
    _, slot = near_slots(nx)
    plane = jnp.where(below_is_first("gx"), nx, 0)
    inner = jnp.where(below_is_first("gx"), nx - WIDTH, 0)
    for layer in range(WIDTH):
        for comp in range(3):
            store_plane(ln, u_ref, comp, slot + layer, second_ref[comp, layer])
    for layer in range(WIDTH):
        for k in range(1, windows):
            filter_z(ln, u_ref, hz_ref, slot + layer, k)
    for layer in range(WIDTH):
        for k in range(1, windows):
            filter_x(hz_ref, hu_ref, plane + layer, k)
    strain_planes(ln, u_ref, mag_ref, tmp_ref, keep_ref, fz_ref, plane, plane + WIDTH)
    sum_planes(ln, hu_ref, fz_ref, acc_ref, inner, inner + WIDTH)


def rim_kernel(
    first_ref, second_ref, _1, _2, _3, _4, _5, acc_ref, u_ref, tmp_ref, hu_ref, mag_ref,
    plain_ref, outer_ref, sums_ref, turned, fz, hz,
):
    planes, _, lanes = u_ref.shape[1:]
    nx = planes - 2 * WIDTH
    ny = lanes // 2
    ln = Lanes(lanes)
    count = first_ref.shape[0]
    upper = lax.broadcasted_iota(jnp.int32, first_ref.shape, 1) >= ny
    take_first = jnp.logical_not(jnp.logical_xor(upper, below_is_first("gz")))
    turned[ROWS : ROWS + count] = pltpu.roll(
        jnp.where(take_first, first_ref[...], second_ref[...]), ny, 1
    )
    for first_row, entries in edge_places(nx):
        for n, (comp, slot) in enumerate(entries):
            at = first_row + WIDTH * (n + 1)
            u_ref[comp, slot, ln.rows(TOP - ROWS)] = turned[ln.rows(at)]
    for slot in range(planes):
        filter_z(ln, u_ref, hz, slot, 0)
    for i in range(nx + 2):
        filter_x(hz, hu_ref, i, 0)
    for i in range(nx + 2):
        strain(ln, u_ref, mag_ref, tmp_ref, None, i, i, 0)
    for i in range(nx + 2):
        filter_products(ln, tmp_ref, fz, i, i, 0)
    carry = acc_ref[0], acc_ref[1]
    for x in range(nx):
        carry = add_sums(ln, hu_ref, fz, x, 0, carry)
    numer, denom = [jnp.sum(part, axis=0, keepdims=True) for part in carry]
    numer = numer + pltpu.roll(numer, ny, 1)
    denom = denom + pltpu.roll(denom, ny, 1)
    both = jnp.where(lax.broadcasted_iota(jnp.int32, (1, lanes), 1) < ny, numer, denom)
    sums_ref[...] = jnp.broadcast_to(both, sums_ref.shape)
    for x in range(nx):
        outer_ref[x : x + 1] = mag_ref[x + 1, 1:2]
    unfold_planes(ln, mag_ref, plain_ref, jnp.where(below_is_first("gx"), nx - 1, 0), 1)


def finish_kernel(cells, parts_ref, mag_ref, outer_ref, coefficient_ref, eddy_ref):
    lanes = parts_ref.shape[1]
    ny = lanes // 2
    sums = jnp.sum(parts_ref[...], axis=0, keepdims=True)
    numer = sums[:, :ny]
    denom = pltpu.roll(sums, ny, 1)[:, :ny]
    coefficient = numer / cells / (denom / cells + 1e-06)
    coefficient_ref[...] = coefficient
    column = jnp.broadcast_to(coefficient, (mag_ref.shape[2], ny)).T
    outer = outer_ref[...].T
    lane = lax.broadcasted_iota(jnp.int32, column.shape, 1)
    for x in range(mag_ref.shape[0]):
        low, high = outer[:ny, x : x + 1], outer[ny:, x : x + 1]
        plane = jnp.where(lane == 0, low, mag_ref[x])
        eddy_ref[x] = column * jnp.where(lane == lane.shape[1] - 1, high, plane)


def call(kernel, shapes, operands, cycles, aliases=None, scratch=()):
    return pl.pallas_call(
        kernel,
        out_shape=tuple(jax.ShapeDtypeStruct(shape, jnp.float32) for shape in shapes),
        in_specs=[VMEM] * len(operands),
        out_specs=tuple(VMEM for _ in shapes),
        scratch_shapes=[
            pltpu.VMEM(item, jnp.float32) if isinstance(item, tuple) else item for item in scratch
        ],
        input_output_aliases=aliases or {},
        compiler_params=pltpu.CompilerParams(vmem_limit_bytes=8 * 1024 * 1024),
        cost_estimate=pl.CostEstimate(
            flops=cycles * 4096, bytes_accessed=0, transcendentals=0
        ),
    )(*operands)


def on_device(velocity):
    nx, ny, nz = velocity.shape[1:]
    half, lanes = nz // 2, 2 * ny
    planes = nx + 2 * WIDTH
    tall, windowed = half + 3 * ROWS, half + ROWS
    u_shape = (3, planes, tall, lanes)
    work = (
        (12, nx + 2, 2 * ROWS, lanes),
        (12, nx + 2, half, lanes),
        (3, planes, windowed, lanes),
        (3, nx + 2, windowed, lanes),
        (nx + 2, windowed, lanes),
        (2, ROWS, lanes),
    )
    window_pair = ((12, 2, windowed, lanes),)
    halo = (3, WIDTH, ny, nz)
    strip_shape = (STRIP, lanes)
    first, second, strip = call(
        load_kernel,
        (halo, halo, strip_shape),
        (velocity,),
        500,
        scratch=((3, WIDTH, 3 * ROWS, lanes),),
    )
    to_first, to_second = swap_axes("gx")
    strip = lax.ppermute(strip, "gx", to_second)
    first = lax.ppermute(first, "gx", to_first)
    second = lax.ppermute(second, "gx", to_second)
    edge_rows = STRIP + WIDTH * 3 * nx + STRIP
    edge_shape = (edge_rows, lanes)
    u, edges = call(fold_kernel, (u_shape, edge_shape), (velocity,), 1200)
    u, edges = call(near_kernel, (u_shape, edge_shape), (first, u, edges), 400, {1: 0, 2: 1})
    (edges,) = call(edge_kernel, (edge_shape,), (strip, edges), 50, {1: 0})
    to_first, to_second = swap_axes("gz")
    low = lax.ppermute(edges, "gz", to_second)
    high = lax.ppermute(edges, "gz", to_first)
    *fields, plain = call(interior_kernel, (*work, (nx, ny, nz)), (u,), 6000, scratch=window_pair)
    u, keep, _, _, hu, mag, acc = call(
        sides_kernel,
        (u_shape, *work),
        (second, u, *fields),
        2000,
        {1 + n: n for n in range(7)},
        window_pair,
    )
    count = lax.axis_size("gx") * lax.axis_size("gz")
    *_, plain, outer, sums = call(
        rim_kernel,
        (u_shape, work[0], work[3], work[4], (nx, ny, nz), (nx, lanes), (count, lanes)),
        (high, low, u, keep, hu, mag, plain, acc),
        1000,
        {2 + n: n for n in range(5)},
        scratch=(
            (ROWS + edge_rows, lanes),
            (12, nx + 2, ROWS, lanes),
            (3, planes, ROWS, lanes),
        ),
    )
    parts = lax.all_to_all(sums, ("gx", "gz"), 0, 0, tiled=True)
    cells = nx * lax.axis_size("gx") * nz * lax.axis_size("gz")
    coefficient, eddy_viscosity = call(
        functools.partial(finish_kernel, cells), ((1, ny), (nx, ny, nz)), (parts, plain, outer), 500
    )
    return (coefficient[0], eddy_viscosity)


def solution(mesh):
    in_specs = (P(None, "gx", None, "gz"),)
    out_specs = (P(), P("gx", None, "gz"))
    return jax.shard_map(
        on_device, mesh=mesh, in_specs=in_specs, out_specs=out_specs, check_vma=False
    )
```

```python
import functools

import jax
import jax.numpy as jnp
from jax import lax
from jax.experimental import pallas as pl
from jax.experimental.pallas import tpu as pltpu
from jax.sharding import PartitionSpec as P


WIDTH = 2
ROWS = 8
index_pairs = ((0, 0), (1, 1), (2, 2), (0, 1), (0, 2), (1, 2))
STRIP = 16
TOP = 9

VMEM = pl.BlockSpec(memory_space=pltpu.VMEM)


def swap_axes(axis):
    count = lax.axis_size(axis)
    if count % 2:
        forward = [(i, (i + 1) % count) for i in range(count)]
        return forward, [(target, source) for source, target in forward]
    far = [(i, (i + 1 if i % 2 else i - 1) % count) for i in range(count)]
    return [(i, i ^ 1) for i in range(count)], far


def below_is_first(axis):
    if lax.axis_size(axis) % 2:
        return True
    return lax.rem(lax.axis_index(axis), 2) == 1


def first_goes_below(axis):
    if lax.axis_size(axis) % 2:
        return False
    return below_is_first(axis)


def mirrored(plane):
    lanes = plane.shape[1]
    lane = lax.broadcasted_iota(jnp.int32, plane.shape, 1)
    return jnp.take_along_axis(plane, lanes - 1 - lane, axis=1)


def to_folded(plane, rows):
    return jnp.concatenate([plane[:, :rows], mirrored(plane)[:, :rows]], axis=0).T


def from_folded(folded):
    half, lanes = folded.shape
    ny = lanes // 2
    turned = folded.T
    both = jnp.concatenate([turned[:ny], turned[ny:]], axis=1)
    lane = lax.broadcasted_iota(jnp.int32, both.shape, 1)
    return jnp.take_along_axis(both, jnp.where(lane < half, lane, 3 * half - 1 - lane), axis=1)


class Lanes:
    def __init__(self, lanes):
        self.zero = jnp.minimum(lax.axis_index("gx"), 0)
        lane = lax.broadcasted_iota(jnp.int32, (ROWS, lanes), 1)
        row_y = lax.rem(lane, lanes // 2)
        self.first, self.last = row_y == 0, row_y == lanes // 2 - 1
        self.scale = jnp.where(self.first | self.last, 2.0, 1.0).astype(jnp.float32)
        self.sign = jnp.where(lane < lanes // 2, 1.0, -1.0).astype(jnp.float32)

    def rows(self, start, count=ROWS):
        return pl.ds(self.zero + start, count)

    def slope_y(self, field):
        lanes = field.shape[1]
        up = jnp.where(self.last, field, pltpu.roll(field, lanes - 1, 1))
        down = jnp.where(self.first, field, pltpu.roll(field, 1, 1))
        return (up - down) * self.scale

    def slope_z(self, after, before):
        return (after - before) * self.sign


def window(k):
    return pl.ds(ROWS * k, ROWS)


def store_plane(ln, u_ref, comp, slot, plane):
    count = plane.shape[1] // 2 + ROWS
    folded = to_folded(plane, count)
    for k in range(count // ROWS):
        u_ref[comp, slot, ln.rows(TOP + ROWS * k)] = folded[ROWS * k : ROWS * (k + 1)]


def rates(slopes):
    rate = [
        slopes[i][i] if i == j else slopes[i][j] + slopes[j][i] for i, j in index_pairs
    ]
    squares = [r * r for r in rate]
    straight = squares[0] + squares[1] + squares[2]
    crossed = squares[3] + squares[4] + squares[5]
    return rate, 0.5 * jnp.sqrt((straight + straight) + crossed)


def weighted(low, mid, high):
    return (low + high) + (mid + mid)


def filter_z(ln, u_ref, hz_ref, slot, k):
    at = ROWS * (k + 1)
    for comp in range(3):
        hz_ref[comp, slot, window(k)] = weighted(
            *[u_ref[comp, slot, ln.rows(at + step)] for step in (-1, 0, 1)]
        )


def strain(ln, u_ref, mag_ref, tmp_ref, keep_ref, slot, i, k, hz_ref=None):
    at = ROWS * (k + 1)
    before, mid, after = [
        [u_ref[comp, i + 1, ln.rows(at + step)] for comp in range(3)] for step in (-1, 0, 1)
    ]
    slopes = [
        (
            u_ref[comp, i + 2, ln.rows(at)] - u_ref[comp, i, ln.rows(at)],
            ln.slope_y(mid[comp]),
            ln.slope_z(after[comp], before[comp]),
        )
        for comp in range(3)
    ]
    if hz_ref is not None:
        for comp in range(3):
            hz_ref[comp, i + 1, window(k)] = weighted(before[comp], mid[comp], after[comp])
    rate, size = rates(slopes)
    mag_ref[i, window(k)] = size
    scaled = size * 0.0625
    quarter = [0.25 * m for m in mid]
    for n, (a, b) in enumerate(index_pairs):
        for at, value in ((n, scaled * rate[n]), (6 + n, quarter[a] * quarter[b])):
            tmp_ref[at, slot, window(k)] = value
            if k == 1:
                keep_ref[at, i, window(1)] = value


def outer_size(ln, u_ref, mag_ref, i):
    at = TOP + 1
    slopes = [
        (
            u_ref[comp, i + 2, ln.rows(at)] - u_ref[comp, i, ln.rows(at)],
            ln.slope_y(u_ref[comp, i + 1, ln.rows(at)]),
            ln.slope_z(u_ref[comp, i + 1, ln.rows(at + 1)], u_ref[comp, i + 1, ln.rows(at - 1)]),
        )
        for comp in range(3)
    ]
    mag_ref[i, ln.rows(2)] = rates(slopes)[1]


def unfold_planes(ln, mag_ref, plain_ref, start, count):
    half = plain_ref.shape[2] // 2
    for n in range(count):
        plain_ref[start + n] = from_folded(mag_ref[start + n + 1, ln.rows(1, half)])


def filter_products(ln, tmp_ref, fz_ref, slot, i, k):
    for n in range(12):
        fz_ref[n, i, window(k)] = weighted(
            *[tmp_ref[n, slot, ln.rows(ROWS * k + step)] for step in (0, 1, 2)]
        )


def filter_x(hz_ref, hu_ref, i, k):
    for comp in range(3):
        hu_ref[comp, i, window(k)] = 0.0625 * weighted(
            *[hz_ref[comp, i + step, window(k)] for step in (0, 1, 2)]
        )


def add_sums(ln, hu_ref, fz_ref, x, k, carry):
    numer, denom = carry
    at = 1 + ROWS * k
    mid = [hu_ref[comp, x + 1, ln.rows(at)] for comp in range(3)]
    slopes = [
        (
            hu_ref[comp, x + 2, ln.rows(at)] - hu_ref[comp, x, ln.rows(at)],
            ln.slope_y(mid[comp]),
            ln.slope_z(
                hu_ref[comp, x + 1, ln.rows(at + 1)], hu_ref[comp, x + 1, ln.rows(at - 1)]
            ),
        )
        for comp in range(3)
    ]
    rate, size = rates(slopes)
    size = 4.0 * size
    top, straight, crossed = [], [], []
    for n, (a, b) in enumerate(index_pairs):
        stress = weighted(*[fz_ref[n, x + step, window(k)] for step in (0, 1, 2)])
        product = weighted(*[fz_ref[6 + n, x + step, window(k)] for step in (0, 1, 2)])
        model = stress - size * rate[n]
        leonard = product - mid[a] * mid[b]
        top.append(leonard * model)
        (straight if a == b else crossed).append(model * model)
    numer = numer + ((top[0] + top[1]) + (top[2] + top[3]) + (top[4] + top[5]))
    denom = denom + (
        (straight[0] + straight[1] + straight[2])
        + 0.5 * (crossed[0] + crossed[1] + crossed[2])
    )
    return numer, denom


def strain_planes(
    ln, u_ref, mag_ref, tmp_ref, keep_ref, fz_ref, start, stop, hz_ref=None
):
    windows = mag_ref.shape[1] // ROWS

    def plane(i):
        if hz_ref is not None:
            outer_size(ln, u_ref, mag_ref, i)
        for k in range(1, windows):
            strain(ln, u_ref, mag_ref, tmp_ref, keep_ref, lax.rem(i, 2), i, k, hz_ref)

    def products(i):
        for k in range(1, windows - 1):
            filter_products(ln, tmp_ref, fz_ref, lax.rem(i, 2), i, k)

    def step(i, carry):
        products(i - 1)
        plane(i)
        return carry

    plane(start)
    lax.fori_loop(start + 1, stop, step, 0)
    products(stop - 1)


def sum_planes(ln, hu_ref, fz_ref, acc_ref, start, stop, beside=None):
    def step(x, carry):
        if beside is not None:
            beside(x)
        for k in range(1, fz_ref.shape[2] // ROWS):
            carry = add_sums(ln, hu_ref, fz_ref, x, k, carry)
        return carry

    acc_ref[0], acc_ref[1] = lax.fori_loop(start, stop, step, (acc_ref[0], acc_ref[1]))


def pack_edges(ln, u_ref, entries):
    packed = None
    for n, (comp, slot) in enumerate(entries):
        for layer in range(WIDTH):
            to = WIDTH * n + WIDTH - 1 - layer
            rows = u_ref[comp, slot, ln.rows(TOP + layer - to)]
            row = lax.broadcasted_iota(jnp.int32, rows.shape, 0)
            packed = rows if packed is None else jnp.where(row == to, rows, packed)
    return packed


def pack_all(ln, u_ref, entries, edge_ref, start):
    for at in range(0, len(entries), ROWS // WIDTH):
        to = start + WIDTH * at
        edge_ref[to : to + ROWS] = pack_edges(ln, u_ref, entries[at : at + ROWS // WIDTH])


def load_kernel(vel_ref, first_ref, second_ref, strip_ref, top_ref):
    nx = vel_ref.shape[1]
    ln = Lanes(strip_ref.shape[1])
    flag = first_goes_below("gx")
    entries = [(comp, layer) for comp in range(3) for layer in range(WIDTH)]
    for comp, layer in entries:
        low, high = vel_ref[comp, layer], vel_ref[comp, nx - WIDTH + layer]
        first_ref[comp, layer] = jnp.where(flag, low, high)
        second = jnp.where(flag, high, low)
        second_ref[comp, layer] = second
        top_ref[comp, layer, ln.rows(TOP)] = to_folded(second, ROWS)
    pack_all(ln, top_ref, entries, strip_ref, 0)


def near_slots(nx):
    flag = below_is_first("gx")
    return jnp.where(flag, 0, WIDTH), jnp.where(flag, nx + WIDTH, 0)


def edge_places(nx):
    start, far = near_slots(nx)
    near = jnp.where(below_is_first("gx"), start, nx + WIDTH)
    block = [(comp, WIDTH + x) for comp in range(3) for x in range(nx)]
    halos = [
        [(comp, slot + layer) for comp in range(3) for layer in range(WIDTH)]
        for slot in (far, near)
    ]
    return ((0, halos[0]), (STRIP, block), (STRIP + WIDTH * len(block), halos[1]))


def fold_kernel(vel_ref, u_ref, edge_ref):
    nx = vel_ref.shape[1]
    ln = Lanes(u_ref.shape[3])

    def fold(x, carry):
        for comp in range(3):
            store_plane(ln, u_ref, comp, WIDTH + x, vel_ref[comp, x])
        return carry

    lax.fori_loop(0, nx, fold, 0, unroll=4)
    row, entries = edge_places(nx)[1]
    pack_all(ln, u_ref, entries, edge_ref, row)


def near_kernel(first_ref, _0, _1, u_ref, edge_ref):
    nx = u_ref.shape[1] - 2 * WIDTH
    ln = Lanes(u_ref.shape[3])
    row, entries = edge_places(nx)[2]
    for n, (comp, slot) in enumerate(entries):
        store_plane(ln, u_ref, comp, slot, first_ref[comp, n % WIDTH])
    pack_all(ln, u_ref, entries, edge_ref, row)


def edge_kernel(strip_ref, _, edge_ref):
    edge_ref[:STRIP] = strip_ref[...]


def interior_kernel(
    u_ref, keep_ref, fz_ref, hz_ref, hu_ref, mag_ref, acc_ref, plain_ref, tmp_ref
):
    nx = u_ref.shape[1] - 2 * WIDTH
    windows = mag_ref.shape[1] // ROWS
    ln = Lanes(u_ref.shape[3])
    start, _ = near_slots(nx)

    for slot in (start, start + nx + 1):
        for k in range(1, windows):
            filter_z(ln, u_ref, hz_ref, slot, k)
    strain_planes(ln, u_ref, mag_ref, tmp_ref, keep_ref, fz_ref, start, start + nx, hz_ref)

    def hat_x(i, carry):
        for k in range(1, windows):
            filter_x(hz_ref, hu_ref, i, k)
        return carry

    lax.fori_loop(start, start + nx, hat_x, 0)
    acc_ref[...] = jnp.zeros_like(acc_ref)
    inner = jnp.maximum(start - 1, 0)

    def unfold(x):
        unfold_planes(ln, mag_ref, plain_ref, inner + x - start, 1)

    sum_planes(ln, hu_ref, fz_ref, acc_ref, start, start + nx - WIDTH, unfold)
    unfold_planes(ln, mag_ref, plain_ref, inner + nx - WIDTH, 1)


def sides_kernel(
    second_ref, _0, _1, _2, _3, _4, _5, _6,
    u_ref, keep_ref, fz_ref, hz_ref, hu_ref, mag_ref, acc_ref, tmp_ref,
):
    nx = u_ref.shape[1] - 2 * WIDTH
    windows = mag_ref.shape[1] // ROWS
    ln = Lanes(u_ref.shape[3])
    _, slot = near_slots(nx)
    plane = jnp.where(below_is_first("gx"), nx, 0)
    inner = jnp.where(below_is_first("gx"), nx - WIDTH, 0)
    for layer in range(WIDTH):
        for comp in range(3):
            store_plane(ln, u_ref, comp, slot + layer, second_ref[comp, layer])
    for layer in range(WIDTH):
        for k in range(1, windows):
            filter_z(ln, u_ref, hz_ref, slot + layer, k)
    for layer in range(WIDTH):
        for k in range(1, windows):
            filter_x(hz_ref, hu_ref, plane + layer, k)
    strain_planes(ln, u_ref, mag_ref, tmp_ref, keep_ref, fz_ref, plane, plane + WIDTH)
    sum_planes(ln, hu_ref, fz_ref, acc_ref, inner, inner + WIDTH)


def rim_kernel(
    first_ref, second_ref, _1, _2, _3, _4, _5, acc_ref, u_ref, tmp_ref, hu_ref, mag_ref,
    plain_ref, outer_ref, sums_ref, turned, fz, hz,
):
    planes, _, lanes = u_ref.shape[1:]
    nx = planes - 2 * WIDTH
    ny = lanes // 2
    ln = Lanes(lanes)
    count = first_ref.shape[0]
    upper = lax.broadcasted_iota(jnp.int32, first_ref.shape, 1) >= ny
    take_first = jnp.logical_not(jnp.logical_xor(upper, below_is_first("gz")))
    turned[ROWS : ROWS + count] = pltpu.roll(
        jnp.where(take_first, first_ref[...], second_ref[...]), ny, 1
    )
    for first_row, entries in edge_places(nx):
        for n, (comp, slot) in enumerate(entries):
            at = first_row + WIDTH * (n + 1)
            u_ref[comp, slot, ln.rows(TOP - ROWS)] = turned[ln.rows(at)]
    for slot in range(planes):
        filter_z(ln, u_ref, hz, slot, 0)
    for i in range(nx + 2):
        filter_x(hz, hu_ref, i, 0)
    for i in range(nx + 2):
        strain(ln, u_ref, mag_ref, tmp_ref, None, i, i, 0)
    for i in range(nx + 2):
        filter_products(ln, tmp_ref, fz, i, i, 0)
    carry = acc_ref[0], acc_ref[1]
    for x in range(nx):
        carry = add_sums(ln, hu_ref, fz, x, 0, carry)
    numer, denom = [jnp.sum(part, axis=0, keepdims=True) for part in carry]
    numer = numer + pltpu.roll(numer, ny, 1)
    denom = denom + pltpu.roll(denom, ny, 1)
    both = jnp.where(lax.broadcasted_iota(jnp.int32, (1, lanes), 1) < ny, numer, denom)
    sums_ref[...] = jnp.broadcast_to(both, sums_ref.shape)
    for x in range(nx):
        outer_ref[x : x + 1] = mag_ref[x + 1, 1:2]
    unfold_planes(ln, mag_ref, plain_ref, jnp.where(below_is_first("gx"), nx - 1, 0), 1)


def finish_kernel(cells, parts_ref, mag_ref, outer_ref, coefficient_ref, eddy_ref):
    lanes = parts_ref.shape[1]
    ny = lanes // 2
    sums = jnp.sum(parts_ref[...], axis=0, keepdims=True)
    numer = sums[:, :ny]
    denom = pltpu.roll(sums, ny, 1)[:, :ny]
    coefficient = numer / cells / (denom / cells + 1e-06)
    coefficient_ref[...] = coefficient
    column = jnp.broadcast_to(coefficient, (mag_ref.shape[2], ny)).T
    outer = outer_ref[...].T
    lane = lax.broadcasted_iota(jnp.int32, column.shape, 1)
    for x in range(mag_ref.shape[0]):
        low, high = outer[:ny, x : x + 1], outer[ny:, x : x + 1]
        plane = jnp.where(lane == 0, low, mag_ref[x])
        eddy_ref[x] = column * jnp.where(lane == lane.shape[1] - 1, high, plane)


def call(kernel, shapes, operands, cycles, aliases=None, scratch=()):
    return pl.pallas_call(
        kernel,
        out_shape=tuple(jax.ShapeDtypeStruct(shape, jnp.float32) for shape in shapes),
        in_specs=[VMEM] * len(operands),
        out_specs=tuple(VMEM for _ in shapes),
        scratch_shapes=[
            pltpu.VMEM(item, jnp.float32) if isinstance(item, tuple) else item for item in scratch
        ],
        input_output_aliases=aliases or {},
        compiler_params=pltpu.CompilerParams(vmem_limit_bytes=8 * 1024 * 1024),
        cost_estimate=pl.CostEstimate(
            flops=cycles * 4096, bytes_accessed=0, transcendentals=0
        ),
    )(*operands)


def on_device(velocity):
    nx, ny, nz = velocity.shape[1:]
    half, lanes = nz // 2, 2 * ny
    planes = nx + 2 * WIDTH
    tall, windowed = half + 3 * ROWS, half + ROWS
    u_shape = (3, planes, tall, lanes)
    work = (
        (12, nx + 2, 2 * ROWS, lanes),
        (12, nx + 2, half, lanes),
        (3, planes, windowed, lanes),
        (3, nx + 2, windowed, lanes),
        (nx + 2, windowed, lanes),
        (2, ROWS, lanes),
    )
    window_pair = ((12, 2, windowed, lanes),)
    halo = (3, WIDTH, ny, nz)
    strip_shape = (STRIP, lanes)
    first, second, strip = call(
        load_kernel,
        (halo, halo, strip_shape),
        (velocity,),
        500,
        scratch=((3, WIDTH, 3 * ROWS, lanes),),
    )
    to_first, to_second = swap_axes("gx")
    strip = lax.ppermute(strip, "gx", to_second)
    first = lax.ppermute(first, "gx", to_first)
    second = lax.ppermute(second, "gx", to_second)
    edge_rows = STRIP + WIDTH * 3 * nx + STRIP
    edge_shape = (edge_rows, lanes)
    u, edges = call(fold_kernel, (u_shape, edge_shape), (velocity,), 1200)
    u, edges = call(near_kernel, (u_shape, edge_shape), (first, u, edges), 400, {1: 0, 2: 1})
    (edges,) = call(edge_kernel, (edge_shape,), (strip, edges), 50, {1: 0})
    to_first, to_second = swap_axes("gz")
    low = lax.ppermute(edges, "gz", to_second)
    high = lax.ppermute(edges, "gz", to_first)
    *fields, plain = call(interior_kernel, (*work, (nx, ny, nz)), (u,), 6000, scratch=window_pair)
    u, keep, _, _, hu, mag, acc = call(
        sides_kernel,
        (u_shape, *work),
        (second, u, *fields),
        2000,
        {1 + n: n for n in range(7)},
        window_pair,
    )
    count = lax.axis_size("gx") * lax.axis_size("gz")
    *_, plain, outer, sums = call(
        rim_kernel,
        (u_shape, work[0], work[3], work[4], (nx, ny, nz), (nx, lanes), (count, lanes)),
        (high, low, u, keep, hu, mag, plain, acc),
        1000,
        {2 + n: n for n in range(5)},
        scratch=(
            (ROWS + edge_rows, lanes),
            (12, nx + 2, ROWS, lanes),
            (3, planes, ROWS, lanes),
        ),
    )
    parts = lax.all_to_all(sums, ("gx", "gz"), 0, 0, tiled=True)
    cells = nx * lax.axis_size("gx") * nz * lax.axis_size("gz")
    coefficient, eddy_viscosity = call(
        functools.partial(finish_kernel, cells), ((1, ny), (nx, ny, nz)), (parts, plain, outer), 500
    )
    return (coefficient[0], eddy_viscosity)


def solution(mesh):
    in_specs = (P(None, "gx", None, "gz"),)
    out_specs = (P(), P("gx", None, "gz"))
    return jax.shard_map(
        on_device, mesh=mesh, in_specs=in_specs, out_specs=out_specs, check_vma=False
    )
```

```python
import functools

import jax
import jax.numpy as jnp
from jax import lax
from jax.experimental import pallas as pl
from jax.experimental.pallas import tpu as pltpu
from jax.sharding import PartitionSpec as P


WIDTH = 2
ROWS = 8
index_pairs = ((0, 0), (1, 1), (2, 2), (0, 1), (0, 2), (1, 2))
STRIP = 16
TOP = 9

VMEM = pl.BlockSpec(memory_space=pltpu.VMEM)


def swap_axes(axis):
    count = lax.axis_size(axis)
    if count % 2:
        forward = [(i, (i + 1) % count) for i in range(count)]
        return forward, [(target, source) for source, target in forward]
    far = [(i, (i + 1 if i % 2 else i - 1) % count) for i in range(count)]
    return [(i, i ^ 1) for i in range(count)], far


def below_is_first(axis):
    if lax.axis_size(axis) % 2:
        return True
    return lax.rem(lax.axis_index(axis), 2) == 1


def first_goes_below(axis):
    if lax.axis_size(axis) % 2:
        return False
    return below_is_first(axis)


def mirrored(plane):
    lanes = plane.shape[1]
    lane = lax.broadcasted_iota(jnp.int32, plane.shape, 1)
    return jnp.take_along_axis(plane, lanes - 1 - lane, axis=1)


def to_folded(plane, rows):
    return jnp.concatenate([plane[:, :rows], mirrored(plane)[:, :rows]], axis=0).T


def from_folded(folded):
    half, lanes = folded.shape
    ny = lanes // 2
    turned = folded.T
    both = jnp.concatenate([turned[:ny], turned[ny:]], axis=1)
    lane = lax.broadcasted_iota(jnp.int32, both.shape, 1)
    return jnp.take_along_axis(both, jnp.where(lane < half, lane, 3 * half - 1 - lane), axis=1)


class Lanes:
    def __init__(self, lanes):
        self.zero = jnp.minimum(lax.axis_index("gx"), 0)
        lane = lax.broadcasted_iota(jnp.int32, (ROWS, lanes), 1)
        row_y = lax.rem(lane, lanes // 2)
        self.first, self.last = row_y == 0, row_y == lanes // 2 - 1
        self.scale = jnp.where(self.first | self.last, 2.0, 1.0).astype(jnp.float32)
        self.sign = jnp.where(lane < lanes // 2, 1.0, -1.0).astype(jnp.float32)

    def rows(self, start, count=ROWS):
        return pl.ds(self.zero + start, count)

    def slope_y(self, field):
        lanes = field.shape[1]
        up = jnp.where(self.last, field, pltpu.roll(field, lanes - 1, 1))
        down = jnp.where(self.first, field, pltpu.roll(field, 1, 1))
        return (up - down) * self.scale

    def slope_z(self, after, before):
        return (after - before) * self.sign


def window(k):
    return pl.ds(ROWS * k, ROWS)


def store_plane(ln, u_ref, comp, slot, plane):
    count = plane.shape[1] // 2 + ROWS
    folded = to_folded(plane, count)
    for k in range(count // ROWS):
        u_ref[comp, slot, ln.rows(TOP + ROWS * k)] = folded[ROWS * k : ROWS * (k + 1)]


def rates(slopes):
    rate = [
        slopes[i][i] if i == j else slopes[i][j] + slopes[j][i] for i, j in index_pairs
    ]
    squares = [r * r for r in rate]
    straight = squares[0] + squares[1] + squares[2]
    crossed = squares[3] + squares[4] + squares[5]
    return rate, 0.5 * jnp.sqrt((straight + straight) + crossed)


def weighted(low, mid, high):
    return (low + high) + (mid + mid)


def filter_z(ln, u_ref, hz_ref, slot, k):
    at = ROWS * (k + 1)
    for comp in range(3):
        hz_ref[comp, slot, window(k)] = weighted(
            *[u_ref[comp, slot, ln.rows(at + step)] for step in (-1, 0, 1)]
        )


def strain(ln, u_ref, mag_ref, tmp_ref, keep_ref, slot, i, k, hz_ref=None):
    at = ROWS * (k + 1)
    before, mid, after = [
        [u_ref[comp, i + 1, ln.rows(at + step)] for comp in range(3)] for step in (-1, 0, 1)
    ]
    slopes = [
        (
            u_ref[comp, i + 2, ln.rows(at)] - u_ref[comp, i, ln.rows(at)],
            ln.slope_y(mid[comp]),
            ln.slope_z(after[comp], before[comp]),
        )
        for comp in range(3)
    ]
    if hz_ref is not None:
        for comp in range(3):
            hz_ref[comp, i + 1, window(k)] = weighted(before[comp], mid[comp], after[comp])
    rate, size = rates(slopes)
    mag_ref[i, window(k)] = size
    scaled = size * 0.0625
    quarter = [0.25 * m for m in mid]
    for n, (a, b) in enumerate(index_pairs):
        for at, value in ((n, scaled * rate[n]), (6 + n, quarter[a] * quarter[b])):
            tmp_ref[at, slot, window(k)] = value
            if k == 1:
                keep_ref[at, i, window(1)] = value


def outer_size(ln, u_ref, mag_ref, i):
    at = TOP + 1
    slopes = [
        (
            u_ref[comp, i + 2, ln.rows(at)] - u_ref[comp, i, ln.rows(at)],
            ln.slope_y(u_ref[comp, i + 1, ln.rows(at)]),
            ln.slope_z(u_ref[comp, i + 1, ln.rows(at + 1)], u_ref[comp, i + 1, ln.rows(at - 1)]),
        )
        for comp in range(3)
    ]
    mag_ref[i, ln.rows(2)] = rates(slopes)[1]


def unfold_planes(ln, mag_ref, plain_ref, start, count):
    half = plain_ref.shape[2] // 2
    for n in range(count):
        plain_ref[start + n] = from_folded(mag_ref[start + n + 1, ln.rows(1, half)])


def filter_products(ln, tmp_ref, fz_ref, slot, i, k):
    for n in range(12):
        fz_ref[n, i, window(k)] = weighted(
            *[tmp_ref[n, slot, ln.rows(ROWS * k + step)] for step in (0, 1, 2)]
        )


def filter_x(hz_ref, hu_ref, i, k):
    for comp in range(3):
        hu_ref[comp, i, window(k)] = 0.0625 * weighted(
            *[hz_ref[comp, i + step, window(k)] for step in (0, 1, 2)]
        )


def add_sums(ln, hu_ref, fz_ref, x, k, carry):
    numer, denom = carry
    at = 1 + ROWS * k
    mid = [hu_ref[comp, x + 1, ln.rows(at)] for comp in range(3)]
    slopes = [
        (
            hu_ref[comp, x + 2, ln.rows(at)] - hu_ref[comp, x, ln.rows(at)],
            ln.slope_y(mid[comp]),
            ln.slope_z(
                hu_ref[comp, x + 1, ln.rows(at + 1)], hu_ref[comp, x + 1, ln.rows(at - 1)]
            ),
        )
        for comp in range(3)
    ]
    rate, size = rates(slopes)
    size = 4.0 * size
    top, straight, crossed = [], [], []
    for n, (a, b) in enumerate(index_pairs):
        stress = weighted(*[fz_ref[n, x + step, window(k)] for step in (0, 1, 2)])
        product = weighted(*[fz_ref[6 + n, x + step, window(k)] for step in (0, 1, 2)])
        model = stress - size * rate[n]
        leonard = product - mid[a] * mid[b]
        top.append(leonard * model)
        (straight if a == b else crossed).append(model * model)
    numer = numer + ((top[0] + top[1]) + (top[2] + top[3]) + (top[4] + top[5]))
    denom = denom + (
        (straight[0] + straight[1] + straight[2])
        + 0.5 * (crossed[0] + crossed[1] + crossed[2])
    )
    return numer, denom


def strain_planes(
    ln, u_ref, mag_ref, tmp_ref, keep_ref, fz_ref, start, stop, hz_ref=None
):
    windows = mag_ref.shape[1] // ROWS

    def plane(i):
        if hz_ref is not None:
            outer_size(ln, u_ref, mag_ref, i)
        for k in range(1, windows):
            strain(ln, u_ref, mag_ref, tmp_ref, keep_ref, lax.rem(i, 2), i, k, hz_ref)

    def products(i):
        for k in range(1, windows - 1):
            filter_products(ln, tmp_ref, fz_ref, lax.rem(i, 2), i, k)

    def step(i, carry):
        products(i - 1)
        plane(i)
        return carry

    plane(start)
    lax.fori_loop(start + 1, stop, step, 0)
    products(stop - 1)


def sum_planes(ln, hu_ref, fz_ref, acc_ref, start, stop, beside=None):
    def step(x, carry):
        if beside is not None:
            beside(x)
        for k in range(1, fz_ref.shape[2] // ROWS):
            carry = add_sums(ln, hu_ref, fz_ref, x, k, carry)
        return carry

    acc_ref[0], acc_ref[1] = lax.fori_loop(start, stop, step, (acc_ref[0], acc_ref[1]))


def pack_edges(ln, u_ref, entries):
    packed = None
    for n, (comp, slot) in enumerate(entries):
        for layer in range(WIDTH):
            to = WIDTH * n + WIDTH - 1 - layer
            rows = u_ref[comp, slot, ln.rows(TOP + layer - to)]
            row = lax.broadcasted_iota(jnp.int32, rows.shape, 0)
            packed = rows if packed is None else jnp.where(row == to, rows, packed)
    return packed


def pack_all(ln, u_ref, entries, edge_ref, start):
    for at in range(0, len(entries), ROWS // WIDTH):
        to = start + WIDTH * at
        edge_ref[to : to + ROWS] = pack_edges(ln, u_ref, entries[at : at + ROWS // WIDTH])


def load_kernel(vel_ref, first_ref, second_ref, strip_ref, top_ref):
    nx = vel_ref.shape[1]
    ln = Lanes(strip_ref.shape[1])
    flag = first_goes_below("gx")
    entries = [(comp, layer) for comp in range(3) for layer in range(WIDTH)]
    for comp, layer in entries:
        low, high = vel_ref[comp, layer], vel_ref[comp, nx - WIDTH + layer]
        first_ref[comp, layer] = jnp.where(flag, low, high)
        second = jnp.where(flag, high, low)
        second_ref[comp, layer] = second
        top_ref[comp, layer, ln.rows(TOP)] = to_folded(second, ROWS)
    pack_all(ln, top_ref, entries, strip_ref, 0)


def near_slots(nx):
    flag = below_is_first("gx")
    return jnp.where(flag, 0, WIDTH), jnp.where(flag, nx + WIDTH, 0)


def edge_places(nx):
    start, far = near_slots(nx)
    near = jnp.where(below_is_first("gx"), start, nx + WIDTH)
    block = [(comp, WIDTH + x) for comp in range(3) for x in range(nx)]
    halos = [
        [(comp, slot + layer) for comp in range(3) for layer in range(WIDTH)]
        for slot in (far, near)
    ]
    return ((0, halos[0]), (STRIP, block), (STRIP + WIDTH * len(block), halos[1]))


def fold_kernel(vel_ref, u_ref, edge_ref):
    nx = vel_ref.shape[1]
    ln = Lanes(u_ref.shape[3])

    def fold(x, carry):
        for comp in range(3):
            store_plane(ln, u_ref, comp, WIDTH + x, vel_ref[comp, x])
        return carry

    lax.fori_loop(0, nx, fold, 0, unroll=4)
    row, entries = edge_places(nx)[1]
    pack_all(ln, u_ref, entries, edge_ref, row)


def near_kernel(first_ref, _0, _1, u_ref, edge_ref):
    nx = u_ref.shape[1] - 2 * WIDTH
    ln = Lanes(u_ref.shape[3])
    row, entries = edge_places(nx)[2]
    for n, (comp, slot) in enumerate(entries):
        store_plane(ln, u_ref, comp, slot, first_ref[comp, n % WIDTH])
    pack_all(ln, u_ref, entries, edge_ref, row)


def edge_kernel(strip_ref, _, edge_ref):
    edge_ref[:STRIP] = strip_ref[...]


def interior_kernel(
    u_ref, keep_ref, fz_ref, hz_ref, hu_ref, mag_ref, acc_ref, plain_ref, tmp_ref
):
    nx = u_ref.shape[1] - 2 * WIDTH
    windows = mag_ref.shape[1] // ROWS
    ln = Lanes(u_ref.shape[3])
    start, _ = near_slots(nx)

    for slot in (start, start + nx + 1):
        for k in range(1, windows):
            filter_z(ln, u_ref, hz_ref, slot, k)
    strain_planes(ln, u_ref, mag_ref, tmp_ref, keep_ref, fz_ref, start, start + nx, hz_ref)

    def hat_x(i, carry):
        for k in range(1, windows):
            filter_x(hz_ref, hu_ref, i, k)
        return carry

    lax.fori_loop(start, start + nx, hat_x, 0)
    acc_ref[...] = jnp.zeros_like(acc_ref)
    inner = jnp.maximum(start - 1, 0)

    def unfold(x):
        unfold_planes(ln, mag_ref, plain_ref, inner + x - start, 1)

    sum_planes(ln, hu_ref, fz_ref, acc_ref, start, start + nx - WIDTH, unfold)
    unfold_planes(ln, mag_ref, plain_ref, inner + nx - WIDTH, 1)


def sides_kernel(
    second_ref, _0, _1, _2, _3, _4, _5, _6,
    u_ref, keep_ref, fz_ref, hz_ref, hu_ref, mag_ref, acc_ref, tmp_ref,
):
    nx = u_ref.shape[1] - 2 * WIDTH
    windows = mag_ref.shape[1] // ROWS
    ln = Lanes(u_ref.shape[3])
    _, slot = near_slots(nx)
    plane = jnp.where(below_is_first("gx"), nx, 0)
    inner = jnp.where(below_is_first("gx"), nx - WIDTH, 0)
    for layer in range(WIDTH):
        for comp in range(3):
            store_plane(ln, u_ref, comp, slot + layer, second_ref[comp, layer])
    for layer in range(WIDTH):
        for k in range(1, windows):
            filter_z(ln, u_ref, hz_ref, slot + layer, k)
    for layer in range(WIDTH):
        for k in range(1, windows):
            filter_x(hz_ref, hu_ref, plane + layer, k)
    strain_planes(ln, u_ref, mag_ref, tmp_ref, keep_ref, fz_ref, plane, plane + WIDTH)
    sum_planes(ln, hu_ref, fz_ref, acc_ref, inner, inner + WIDTH)


def rim_kernel(
    first_ref, second_ref, _1, _2, _3, _4, _5, acc_ref, u_ref, tmp_ref, hu_ref, mag_ref,
    plain_ref, sums_ref, turned, fz, hz, outer_ref,
):
    planes, _, lanes = u_ref.shape[1:]
    nx = planes - 2 * WIDTH
    ny = lanes // 2
    ln = Lanes(lanes)
    count = first_ref.shape[0]
    upper = lax.broadcasted_iota(jnp.int32, first_ref.shape, 1) >= ny
    take_first = jnp.logical_not(jnp.logical_xor(upper, below_is_first("gz")))
    turned[ROWS : ROWS + count] = pltpu.roll(
        jnp.where(take_first, first_ref[...], second_ref[...]), ny, 1
    )
    for first_row, entries in edge_places(nx):
        for n, (comp, slot) in enumerate(entries):
            at = first_row + WIDTH * (n + 1)
            u_ref[comp, slot, ln.rows(TOP - ROWS)] = turned[ln.rows(at)]
    for slot in range(planes):
        filter_z(ln, u_ref, hz, slot, 0)
    for i in range(nx + 2):
        filter_x(hz, hu_ref, i, 0)
    for i in range(nx + 2):
        strain(ln, u_ref, mag_ref, tmp_ref, None, i, i, 0)
    for x in range(nx):
        outer_ref[x : x + 1] = mag_ref[x + 1, 1:2]
    unfold_planes(ln, mag_ref, plain_ref, jnp.where(below_is_first("gx"), nx - 1, 0), 1)
    outer = outer_ref[...].T
    depth = lax.broadcasted_iota(jnp.int32, plain_ref.shape[1:], 1)
    for x in range(nx):
        low, high = outer[:ny, x : x + 1], outer[ny:, x : x + 1]
        plane = jnp.where(depth == 0, low, plain_ref[x])
        plain_ref[x] = jnp.where(depth == depth.shape[1] - 1, high, plane)
    for i in range(nx + 2):
        filter_products(ln, tmp_ref, fz, i, i, 0)
    carry = acc_ref[0], acc_ref[1]
    for x in range(nx):
        carry = add_sums(ln, hu_ref, fz, x, 0, carry)
    numer, denom = [jnp.sum(part, axis=0, keepdims=True) for part in carry]
    numer = numer + pltpu.roll(numer, ny, 1)
    denom = denom + pltpu.roll(denom, ny, 1)
    both = jnp.where(lax.broadcasted_iota(jnp.int32, (1, lanes), 1) < ny, numer, denom)
    sums_ref[...] = jnp.broadcast_to(both, sums_ref.shape)


def finish_kernel(cells, parts_ref, mag_ref, coefficient_ref, eddy_ref):
    lanes = parts_ref.shape[1]
    ny = lanes // 2
    sums = jnp.sum(parts_ref[...], axis=0, keepdims=True)
    numer = sums[:, :ny]
    denom = pltpu.roll(sums, ny, 1)[:, :ny]
    coefficient = numer / cells / (denom / cells + 1e-06)
    coefficient_ref[...] = coefficient
    column = jnp.broadcast_to(coefficient, (mag_ref.shape[2], ny)).T
    for x in range(mag_ref.shape[0]):
        eddy_ref[x] = column * mag_ref[x]


def call(kernel, shapes, operands, cycles, aliases=None, scratch=()):
    return pl.pallas_call(
        kernel,
        out_shape=tuple(jax.ShapeDtypeStruct(shape, jnp.float32) for shape in shapes),
        in_specs=[VMEM] * len(operands),
        out_specs=tuple(VMEM for _ in shapes),
        scratch_shapes=[
            pltpu.VMEM(item, jnp.float32) if isinstance(item, tuple) else item for item in scratch
        ],
        input_output_aliases=aliases or {},
        compiler_params=pltpu.CompilerParams(vmem_limit_bytes=8 * 1024 * 1024),
        cost_estimate=pl.CostEstimate(
            flops=cycles * 4096, bytes_accessed=0, transcendentals=0
        ),
    )(*operands)


def on_device(velocity):
    nx, ny, nz = velocity.shape[1:]
    half, lanes = nz // 2, 2 * ny
    planes = nx + 2 * WIDTH
    tall, windowed = half + 3 * ROWS, half + ROWS
    u_shape = (3, planes, tall, lanes)
    work = (
        (12, nx + 2, 2 * ROWS, lanes),
        (12, nx + 2, half, lanes),
        (3, planes, windowed, lanes),
        (3, nx + 2, windowed, lanes),
        (nx + 2, windowed, lanes),
        (2, ROWS, lanes),
    )
    window_pair = ((12, 2, windowed, lanes),)
    halo = (3, WIDTH, ny, nz)
    strip_shape = (STRIP, lanes)
    first, second, strip = call(
        load_kernel,
        (halo, halo, strip_shape),
        (velocity,),
        500,
        scratch=((3, WIDTH, 3 * ROWS, lanes),),
    )
    to_first, to_second = swap_axes("gx")
    strip = lax.ppermute(strip, "gx", to_second)
    first = lax.ppermute(first, "gx", to_first)
    second = lax.ppermute(second, "gx", to_second)
    edge_rows = STRIP + WIDTH * 3 * nx + STRIP
    edge_shape = (edge_rows, lanes)
    u, edges = call(fold_kernel, (u_shape, edge_shape), (velocity,), 1200)
    u, edges = call(near_kernel, (u_shape, edge_shape), (first, u, edges), 400, {1: 0, 2: 1})
    (edges,) = call(edge_kernel, (edge_shape,), (strip, edges), 50, {1: 0})
    to_first, to_second = swap_axes("gz")
    low = lax.ppermute(edges, "gz", to_second)
    high = lax.ppermute(edges, "gz", to_first)
    *fields, plain = call(interior_kernel, (*work, (nx, ny, nz)), (u,), 6000, scratch=window_pair)
    u, keep, _, _, hu, mag, acc = call(
        sides_kernel,
        (u_shape, *work),
        (second, u, *fields),
        2000,
        {1 + n: n for n in range(7)},
        window_pair,
    )
    count = lax.axis_size("gx") * lax.axis_size("gz")
    *_, plain, sums = call(
        rim_kernel,
        (u_shape, work[0], work[3], work[4], (nx, ny, nz), (count, lanes)),
        (high, low, u, keep, hu, mag, plain, acc),
        1000,
        {2 + n: n for n in range(5)},
        scratch=(
            (ROWS + edge_rows, lanes),
            (12, nx + 2, ROWS, lanes),
            (3, planes, ROWS, lanes),
            (nx, lanes),
        ),
    )
    parts = lax.all_to_all(sums, ("gx", "gz"), 0, 0, tiled=True)
    cells = nx * lax.axis_size("gx") * nz * lax.axis_size("gz")
    coefficient, eddy_viscosity = call(
        functools.partial(finish_kernel, cells), ((1, ny), (nx, ny, nz)), (parts, plain), 500
    )
    return (coefficient[0], eddy_viscosity)


def solution(mesh):
    in_specs = (P(None, "gx", None, "gz"),)
    out_specs = (P(), P("gx", None, "gz"))
    return jax.shard_map(
        on_device, mesh=mesh, in_specs=in_specs, out_specs=out_specs, check_vma=False
    )
```

```python
import functools

import jax
import jax.numpy as jnp
from jax import lax
from jax.experimental import pallas as pl
from jax.experimental.pallas import tpu as pltpu
from jax.sharding import PartitionSpec as P


WIDTH = 2
ROWS = 8
index_pairs = ((0, 0), (1, 1), (2, 2), (0, 1), (0, 2), (1, 2))
STRIP = 16
TOP = 9

VMEM = pl.BlockSpec(memory_space=pltpu.VMEM)


def swap_axes(axis):
    count = lax.axis_size(axis)
    if count % 2:
        forward = [(i, (i + 1) % count) for i in range(count)]
        return forward, [(target, source) for source, target in forward]
    far = [(i, (i + 1 if i % 2 else i - 1) % count) for i in range(count)]
    return [(i, i ^ 1) for i in range(count)], far


def below_is_first(axis):
    if lax.axis_size(axis) % 2:
        return True
    return lax.rem(lax.axis_index(axis), 2) == 1


def first_goes_below(axis):
    if lax.axis_size(axis) % 2:
        return False
    return below_is_first(axis)


def mirrored(plane):
    lanes = plane.shape[1]
    lane = lax.broadcasted_iota(jnp.int32, plane.shape, 1)
    return jnp.take_along_axis(plane, lanes - 1 - lane, axis=1)


def to_folded(plane, rows):
    return jnp.concatenate([plane[:, :rows], mirrored(plane)[:, :rows]], axis=0).T


def from_folded(folded):
    half, lanes = folded.shape
    ny = lanes // 2
    turned = folded.T
    both = jnp.concatenate([turned[:ny], turned[ny:]], axis=1)
    lane = lax.broadcasted_iota(jnp.int32, both.shape, 1)
    return jnp.take_along_axis(both, jnp.where(lane < half, lane, 3 * half - 1 - lane), axis=1)


class Lanes:
    def __init__(self, lanes):
        self.zero = jnp.minimum(lax.axis_index("gx"), 0)
        lane = lax.broadcasted_iota(jnp.int32, (ROWS, lanes), 1)
        row_y = lax.rem(lane, lanes // 2)
        self.first, self.last = row_y == 0, row_y == lanes // 2 - 1
        self.scale = jnp.where(self.first | self.last, 2.0, 1.0).astype(jnp.float32)
        self.sign = jnp.where(lane < lanes // 2, 1.0, -1.0).astype(jnp.float32)

    def rows(self, start, count=ROWS):
        return pl.ds(self.zero + start, count)

    def slope_y(self, field):
        lanes = field.shape[1]
        up = jnp.where(self.last, field, pltpu.roll(field, lanes - 1, 1))
        down = jnp.where(self.first, field, pltpu.roll(field, 1, 1))
        return (up - down) * self.scale

    def slope_z(self, after, before):
        return (after - before) * self.sign


def window(k):
    return pl.ds(ROWS * k, ROWS)


def store_plane(ln, u_ref, comp, slot, plane):
    count = plane.shape[1] // 2 + ROWS
    folded = to_folded(plane, count)
    for k in range(count // ROWS):
        u_ref[comp, slot, ln.rows(TOP + ROWS * k)] = folded[ROWS * k : ROWS * (k + 1)]


def rates(slopes):
    rate = [
        slopes[i][i] if i == j else slopes[i][j] + slopes[j][i] for i, j in index_pairs
    ]
    squares = [r * r for r in rate]
    straight = squares[0] + squares[1] + squares[2]
    crossed = squares[3] + squares[4] + squares[5]
    return rate, 0.5 * jnp.sqrt((straight + straight) + crossed)


def weighted(low, mid, high):
    return (low + high) + (mid + mid)


def filter_z(ln, u_ref, hz_ref, slot, k):
    at = ROWS * (k + 1)
    for comp in range(3):
        hz_ref[comp, slot, window(k)] = weighted(
            *[u_ref[comp, slot, ln.rows(at + step)] for step in (-1, 0, 1)]
        )


def strain(ln, u_ref, mag_ref, tmp_ref, keep_ref, slot, i, k, hz_ref=None):
    at = ROWS * (k + 1)
    before, mid, after = [
        [u_ref[comp, i + 1, ln.rows(at + step)] for comp in range(3)] for step in (-1, 0, 1)
    ]
    slopes = [
        (
            u_ref[comp, i + 2, ln.rows(at)] - u_ref[comp, i, ln.rows(at)],
            ln.slope_y(mid[comp]),
            ln.slope_z(after[comp], before[comp]),
        )
        for comp in range(3)
    ]
    if hz_ref is not None:
        for comp in range(3):
            hz_ref[comp, i + 1, window(k)] = weighted(before[comp], mid[comp], after[comp])
    rate, size = rates(slopes)
    mag_ref[i, window(k)] = size
    scaled = size * 0.0625
    quarter = [0.25 * m for m in mid]
    for n, (a, b) in enumerate(index_pairs):
        for at, value in ((n, scaled * rate[n]), (6 + n, quarter[a] * quarter[b])):
            tmp_ref[at, slot, window(k)] = value
            if k == 1:
                keep_ref[at, i, window(1)] = value


def outer_size(ln, u_ref, mag_ref, i):
    at = TOP + 1
    slopes = [
        (
            u_ref[comp, i + 2, ln.rows(at)] - u_ref[comp, i, ln.rows(at)],
            ln.slope_y(u_ref[comp, i + 1, ln.rows(at)]),
            ln.slope_z(u_ref[comp, i + 1, ln.rows(at + 1)], u_ref[comp, i + 1, ln.rows(at - 1)]),
        )
        for comp in range(3)
    ]
    mag_ref[i, ln.rows(2)] = rates(slopes)[1]


def unfold_planes(ln, mag_ref, plain_ref, start, count):
    half = plain_ref.shape[2] // 2
    for n in range(count):
        plain_ref[start + n] = from_folded(mag_ref[start + n + 1, ln.rows(1, half)])


def filter_products(ln, tmp_ref, fz_ref, slot, i, k):
    for n in range(12):
        fz_ref[n, i, window(k)] = weighted(
            *[tmp_ref[n, slot, ln.rows(ROWS * k + step)] for step in (0, 1, 2)]
        )


def filter_x(hz_ref, hu_ref, i, k):
    for comp in range(3):
        hu_ref[comp, i, window(k)] = 0.0625 * weighted(
            *[hz_ref[comp, i + step, window(k)] for step in (0, 1, 2)]
        )


def add_sums(ln, hu_ref, fz_ref, x, k, carry):
    numer, denom = carry
    at = 1 + ROWS * k
    mid = [hu_ref[comp, x + 1, ln.rows(at)] for comp in range(3)]
    slopes = [
        (
            hu_ref[comp, x + 2, ln.rows(at)] - hu_ref[comp, x, ln.rows(at)],
            ln.slope_y(mid[comp]),
            ln.slope_z(
                hu_ref[comp, x + 1, ln.rows(at + 1)], hu_ref[comp, x + 1, ln.rows(at - 1)]
            ),
        )
        for comp in range(3)
    ]
    rate, size = rates(slopes)
    size = 4.0 * size
    top, straight, crossed = [], [], []
    for n, (a, b) in enumerate(index_pairs):
        stress = weighted(*[fz_ref[n, x + step, window(k)] for step in (0, 1, 2)])
        product = weighted(*[fz_ref[6 + n, x + step, window(k)] for step in (0, 1, 2)])
        model = stress - size * rate[n]
        leonard = product - mid[a] * mid[b]
        top.append(leonard * model)
        (straight if a == b else crossed).append(model * model)
    numer = numer + ((top[0] + top[1]) + (top[2] + top[3]) + (top[4] + top[5]))
    denom = denom + (
        (straight[0] + straight[1] + straight[2])
        + 0.5 * (crossed[0] + crossed[1] + crossed[2])
    )
    return numer, denom


def strain_planes(
    ln, u_ref, mag_ref, tmp_ref, keep_ref, fz_ref, start, stop, hz_ref=None
):
    windows = mag_ref.shape[1] // ROWS

    def plane(i):
        if hz_ref is not None:
            outer_size(ln, u_ref, mag_ref, i)
        for k in range(1, windows):
            strain(ln, u_ref, mag_ref, tmp_ref, keep_ref, lax.rem(i, 2), i, k, hz_ref)

    def products(i):
        for k in range(1, windows - 1):
            filter_products(ln, tmp_ref, fz_ref, lax.rem(i, 2), i, k)

    def step(i, carry):
        products(i - 1)
        plane(i)
        return carry

    plane(start)
    lax.fori_loop(start + 1, stop, step, 0)
    products(stop - 1)


def sum_planes(ln, hu_ref, fz_ref, acc_ref, start, stop, beside=None):
    def step(x, carry):
        if beside is not None:
            beside(x)
        for k in range(1, fz_ref.shape[2] // ROWS):
            carry = add_sums(ln, hu_ref, fz_ref, x, k, carry)
        return carry

    acc_ref[0], acc_ref[1] = lax.fori_loop(start, stop, step, (acc_ref[0], acc_ref[1]))


def pack_edges(ln, u_ref, entries):
    packed = None
    for n, (comp, slot) in enumerate(entries):
        for layer in range(WIDTH):
            to = WIDTH * n + WIDTH - 1 - layer
            rows = u_ref[comp, slot, ln.rows(TOP + layer - to)]
            row = lax.broadcasted_iota(jnp.int32, rows.shape, 0)
            packed = rows if packed is None else jnp.where(row == to, rows, packed)
    return packed


def pack_all(ln, u_ref, entries, edge_ref, start):
    for at in range(0, len(entries), ROWS // WIDTH):
        to = start + WIDTH * at
        edge_ref[to : to + ROWS] = pack_edges(ln, u_ref, entries[at : at + ROWS // WIDTH])


def load_kernel(vel_ref, first_ref, second_ref, strip_ref, top_ref):
    nx = vel_ref.shape[1]
    ln = Lanes(strip_ref.shape[1])
    flag = first_goes_below("gx")
    entries = [(comp, layer) for comp in range(3) for layer in range(WIDTH)]
    for comp, layer in entries:
        low, high = vel_ref[comp, layer], vel_ref[comp, nx - WIDTH + layer]
        first_ref[comp, layer] = jnp.where(flag, low, high)
        second = jnp.where(flag, high, low)
        second_ref[comp, layer] = second
        top_ref[comp, layer, ln.rows(TOP)] = to_folded(second, ROWS)
    pack_all(ln, top_ref, entries, strip_ref, 0)


def near_slots(nx):
    flag = below_is_first("gx")
    return jnp.where(flag, 0, WIDTH), jnp.where(flag, nx + WIDTH, 0)


def edge_places(nx):
    start, far = near_slots(nx)
    near = jnp.where(below_is_first("gx"), start, nx + WIDTH)
    block = [(comp, WIDTH + x) for comp in range(3) for x in range(nx)]
    halos = [
        [(comp, slot + layer) for comp in range(3) for layer in range(WIDTH)]
        for slot in (far, near)
    ]
    return ((0, halos[0]), (STRIP, block), (STRIP + WIDTH * len(block), halos[1]))


def fold_kernel(vel_ref, u_ref, edge_ref):
    nx = vel_ref.shape[1]
    ln = Lanes(u_ref.shape[3])

    def fold(x, carry):
        for comp in range(3):
            store_plane(ln, u_ref, comp, WIDTH + x, vel_ref[comp, x])
        return carry

    lax.fori_loop(0, nx, fold, 0, unroll=4)
    row, entries = edge_places(nx)[1]
    pack_all(ln, u_ref, entries, edge_ref, row)


def near_kernel(first_ref, _0, _1, u_ref, edge_ref):
    nx = u_ref.shape[1] - 2 * WIDTH
    ln = Lanes(u_ref.shape[3])
    row, entries = edge_places(nx)[2]
    for n, (comp, slot) in enumerate(entries):
        store_plane(ln, u_ref, comp, slot, first_ref[comp, n % WIDTH])
    pack_all(ln, u_ref, entries, edge_ref, row)


def edge_kernel(strip_ref, _, edge_ref):
    edge_ref[:STRIP] = strip_ref[...]


def interior_kernel(
    u_ref, keep_ref, fz_ref, hz_ref, hu_ref, mag_ref, acc_ref, plain_ref, tmp_ref
):
    nx = u_ref.shape[1] - 2 * WIDTH
    windows = mag_ref.shape[1] // ROWS
    ln = Lanes(u_ref.shape[3])
    start, _ = near_slots(nx)

    for slot in (start, start + nx + 1):
        for k in range(1, windows):
            filter_z(ln, u_ref, hz_ref, slot, k)
    strain_planes(ln, u_ref, mag_ref, tmp_ref, keep_ref, fz_ref, start, start + nx, hz_ref)

    def hat_x(i, carry):
        for k in range(1, windows):
            filter_x(hz_ref, hu_ref, i, k)
        return carry

    lax.fori_loop(start, start + nx, hat_x, 0)
    acc_ref[...] = jnp.zeros_like(acc_ref)
    inner = jnp.maximum(start - 1, 0)

    def unfold(x):
        unfold_planes(ln, mag_ref, plain_ref, inner + x - start, 1)

    sum_planes(ln, hu_ref, fz_ref, acc_ref, start, start + nx - WIDTH, unfold)
    unfold_planes(ln, mag_ref, plain_ref, inner + nx - WIDTH, 1)


def sides_kernel(
    second_ref, _0, _1, _2, _3, _4, _5, _6,
    u_ref, keep_ref, fz_ref, hz_ref, hu_ref, mag_ref, acc_ref, tmp_ref,
):
    nx = u_ref.shape[1] - 2 * WIDTH
    windows = mag_ref.shape[1] // ROWS
    ln = Lanes(u_ref.shape[3])
    _, slot = near_slots(nx)
    plane = jnp.where(below_is_first("gx"), nx, 0)
    inner = jnp.where(below_is_first("gx"), nx - WIDTH, 0)
    for layer in range(WIDTH):
        for comp in range(3):
            store_plane(ln, u_ref, comp, slot + layer, second_ref[comp, layer])
    for layer in range(WIDTH):
        for k in range(1, windows):
            filter_z(ln, u_ref, hz_ref, slot + layer, k)
    for layer in range(WIDTH):
        for k in range(1, windows):
            filter_x(hz_ref, hu_ref, plane + layer, k)
    strain_planes(ln, u_ref, mag_ref, tmp_ref, keep_ref, fz_ref, plane, plane + WIDTH)
    sum_planes(ln, hu_ref, fz_ref, acc_ref, inner, inner + WIDTH)


def rim_kernel(
    first_ref, second_ref, _1, _2, _3, _4, _5, acc_ref, u_ref, tmp_ref, hu_ref, mag_ref,
    plain_ref, sums_ref, turned, fz, hz, outer_ref,
):
    planes, _, lanes = u_ref.shape[1:]
    nx = planes - 2 * WIDTH
    ny = lanes // 2
    ln = Lanes(lanes)
    count = first_ref.shape[0]
    upper = lax.broadcasted_iota(jnp.int32, first_ref.shape, 1) >= ny
    take_first = jnp.logical_not(jnp.logical_xor(upper, below_is_first("gz")))
    turned[ROWS : ROWS + count] = pltpu.roll(
        jnp.where(take_first, first_ref[...], second_ref[...]), ny, 1
    )
    for first_row, entries in edge_places(nx):
        for n, (comp, slot) in enumerate(entries):
            at = first_row + WIDTH * (n + 1)
            u_ref[comp, slot, ln.rows(TOP - ROWS)] = turned[ln.rows(at)]
    for slot in range(planes):
        filter_z(ln, u_ref, hz, slot, 0)
    for i in range(nx + 2):
        filter_x(hz, hu_ref, i, 0)
    for i in range(nx + 2):
        strain(ln, u_ref, mag_ref, tmp_ref, None, i, i, 0)
    for x in range(nx):
        outer_ref[x : x + 1] = mag_ref[x + 1, 1:2]
    unfold_planes(ln, mag_ref, plain_ref, jnp.where(below_is_first("gx"), nx - 1, 0), 1)
    outer = outer_ref[...].T
    depth = lax.broadcasted_iota(jnp.int32, plain_ref.shape[1:], 1)
    for x in range(nx):
        low, high = outer[:ny, x : x + 1], outer[ny:, x : x + 1]
        plane = jnp.where(depth == 0, low, plain_ref[x])
        plain_ref[x] = jnp.where(depth == depth.shape[1] - 1, high, plane)
    for i in range(nx + 2):
        filter_products(ln, tmp_ref, fz, i, i, 0)
    carry = acc_ref[0], acc_ref[1]
    for x in range(nx):
        carry = add_sums(ln, hu_ref, fz, x, 0, carry)
    numer, denom = [jnp.sum(part, axis=0, keepdims=True) for part in carry]
    row = lax.broadcasted_iota(jnp.int32, sums_ref.shape, 0)
    sums_ref[...] = jnp.where(lax.rem(row, 2) == 0, numer, denom)


def finish_kernel(cells, parts_ref, mag_ref, coefficient_ref, eddy_ref):
    lanes = parts_ref.shape[1]
    ny = lanes // 2
    parts = parts_ref[...]
    even = lax.rem(lax.broadcasted_iota(jnp.int32, parts.shape, 0), 2) == 0
    numer = jnp.sum(jnp.where(even, parts, 0.0), axis=0, keepdims=True)
    denom = jnp.sum(jnp.where(even, 0.0, parts), axis=0, keepdims=True)
    numer = (numer + pltpu.roll(numer, ny, 1))[:, :ny]
    denom = (denom + pltpu.roll(denom, ny, 1))[:, :ny]
    coefficient = numer / cells / (denom / cells + 1e-06)
    coefficient_ref[...] = coefficient
    column = jnp.broadcast_to(coefficient, (mag_ref.shape[2], ny)).T
    for x in range(mag_ref.shape[0]):
        eddy_ref[x] = column * mag_ref[x]


def call(kernel, shapes, operands, cycles, aliases=None, scratch=()):
    return pl.pallas_call(
        kernel,
        out_shape=tuple(jax.ShapeDtypeStruct(shape, jnp.float32) for shape in shapes),
        in_specs=[VMEM] * len(operands),
        out_specs=tuple(VMEM for _ in shapes),
        scratch_shapes=[
            pltpu.VMEM(item, jnp.float32) if isinstance(item, tuple) else item for item in scratch
        ],
        input_output_aliases=aliases or {},
        compiler_params=pltpu.CompilerParams(vmem_limit_bytes=8 * 1024 * 1024),
        cost_estimate=pl.CostEstimate(
            flops=cycles * 4096, bytes_accessed=0, transcendentals=0
        ),
    )(*operands)


def on_device(velocity):
    nx, ny, nz = velocity.shape[1:]
    half, lanes = nz // 2, 2 * ny
    planes = nx + 2 * WIDTH
    tall, windowed = half + 3 * ROWS, half + ROWS
    u_shape = (3, planes, tall, lanes)
    work = (
        (12, nx + 2, 2 * ROWS, lanes),
        (12, nx + 2, half, lanes),
        (3, planes, windowed, lanes),
        (3, nx + 2, windowed, lanes),
        (nx + 2, windowed, lanes),
        (2, ROWS, lanes),
    )
    window_pair = ((12, 2, windowed, lanes),)
    halo = (3, WIDTH, ny, nz)
    strip_shape = (STRIP, lanes)
    first, second, strip = call(
        load_kernel,
        (halo, halo, strip_shape),
        (velocity,),
        500,
        scratch=((3, WIDTH, 3 * ROWS, lanes),),
    )
    to_first, to_second = swap_axes("gx")
    strip = lax.ppermute(strip, "gx", to_second)
    first = lax.ppermute(first, "gx", to_first)
    second = lax.ppermute(second, "gx", to_second)
    edge_rows = STRIP + WIDTH * 3 * nx + STRIP
    edge_shape = (edge_rows, lanes)
    u, edges = call(fold_kernel, (u_shape, edge_shape), (velocity,), 1200)
    u, edges = call(near_kernel, (u_shape, edge_shape), (first, u, edges), 400, {1: 0, 2: 1})
    (edges,) = call(edge_kernel, (edge_shape,), (strip, edges), 50, {1: 0})
    to_first, to_second = swap_axes("gz")
    low = lax.ppermute(edges, "gz", to_second)
    high = lax.ppermute(edges, "gz", to_first)
    *fields, plain = call(interior_kernel, (*work, (nx, ny, nz)), (u,), 6000, scratch=window_pair)
    u, keep, _, _, hu, mag, acc = call(
        sides_kernel,
        (u_shape, *work),
        (second, u, *fields),
        2000,
        {1 + n: n for n in range(7)},
        window_pair,
    )
    count = lax.axis_size("gx") * lax.axis_size("gz")
    *_, plain, sums = call(
        rim_kernel,
        (u_shape, work[0], work[3], work[4], (nx, ny, nz), (2 * count, lanes)),
        (high, low, u, keep, hu, mag, plain, acc),
        1000,
        {2 + n: n for n in range(5)},
        scratch=(
            (ROWS + edge_rows, lanes),
            (12, nx + 2, ROWS, lanes),
            (3, planes, ROWS, lanes),
            (nx, lanes),
        ),
    )
    parts = lax.all_to_all(sums, ("gx", "gz"), 0, 0, tiled=True)
    cells = nx * lax.axis_size("gx") * nz * lax.axis_size("gz")
    coefficient, eddy_viscosity = call(
        functools.partial(finish_kernel, cells), ((1, ny), (nx, ny, nz)), (parts, plain), 500
    )
    return (coefficient[0], eddy_viscosity)


def solution(mesh):
    in_specs = (P(None, "gx", None, "gz"),)
    out_specs = (P(), P("gx", None, "gz"))
    return jax.shard_map(
        on_device, mesh=mesh, in_specs=in_specs, out_specs=out_specs, check_vma=False
    )
```
